32 devices in a mesh: rep: 2 (over x), tp: 4 (over z), pp: 4 (over y, core).
Axes of the slice: x: 2, y: 2, z: 4, core: 2. Of those that a mesh axis runs over, the one named last changes fastest.
Arguments:
- w_gate: bfloat16 [4, 896, 4864], P('pp', None, 'tp')
- w_up: bfloat16 [4, 896, 4864], P('pp', None, 'tp')
- w_down: bfloat16 [4, 4864, 896], P('pp', 'tp')
- norm_gain: bfloat16 [4, 896], P('pp')
- a_up: bfloat16 [4, 12, 896, 32], P('pp', 'rep'), parts along dimension 1
- b_up: bfloat16 [4, 12, 32, 4864], P('pp', 'rep', None, 'tp'), parts along dimension 1
- a_down: bfloat16 [4, 12, 4864, 32], P('pp', 'rep', 'tp'), parts along dimension 1
- b_down: bfloat16 [4, 12, 32, 896], P('pp', 'rep'), parts along dimension 1
- inputs: bfloat16 [12, 3, 2, 64, 896], P('rep'), parts along dimension 0
- targets: bfloat16 [12, 3, 2, 64, 896], P('rep'), parts along dimension 0
- lengths: int32 [12, 3, 2], P('rep'), parts along dimension 0
Outputs:
- output 1: float32 [12], P('rep'), parts along dimension 0
- output 2: float32 [4, 12, 896, 32], P('pp', 'rep'), parts along dimension 1
- output 3: float32 [4, 12, 32, 4864], P('pp', 'rep', None, 'tp'), parts along dimension 1
- output 4: float32 [4, 12, 4864, 32], P('pp', 'rep', 'tp'), parts along dimension 1
- output 5: float32 [4, 12, 32, 896], P('pp', 'rep'), parts along dimension 1
There are 2 independent parts. The reference program is written for one: setup_inputs(seed, part) draws one part's arguments, and reference() takes and returns one part's arrays. A program takes and returns all parts, laid end to end along the dimension named above; an argument that names none is the same for every part.
All inputs are finite; a program needn't handle non-finite values.
Results may differ from the reference program's by a relative error of at most 0.0197842.
Values are sent between devices in bfloat16 or wider.
A program may use at most 1 GiB of HBM per device.

```python
import jax
import jax.numpy as jnp
from jax import lax

D_MODEL = 896
D_FFN = 4864
LORA_RANK = 32
NUM_JOBS = 6
NUM_MICRO = 3
MICRO_ROWS = 2
SEQ_LEN = 64
NUM_LAYERS = 4

LORA_SCALE = 2.0
NORM_EPS = 1e-5
TOKENS_MICRO = MICRO_ROWS * SEQ_LEN


def normal_scaled(rng_key, arr_shape, scale_val):
    return jax.random.normal(rng_key, arr_shape, jnp.float32) * scale_val


def setup_inputs(seed: int = 0, part: int = 0) -> dict:
    base_keys = jax.random.split(jax.random.key(seed), 4)
    part_keys = jax.random.split(jax.random.fold_in(jax.random.key(seed + 1), part), 7)
    down_scale = (2.0 / NUM_LAYERS) ** 0.5
    lengths = jax.random.randint(part_keys[4], (NUM_JOBS, NUM_MICRO, MICRO_ROWS), 1, SEQ_LEN + 1, jnp.int32)
    lengths = lengths.at[0, 0, 0].set(SEQ_LEN)
    data_shape = (NUM_JOBS, NUM_MICRO, MICRO_ROWS, SEQ_LEN, D_MODEL)
    return {
        "w_gate": normal_scaled(base_keys[0], (NUM_LAYERS, D_MODEL, D_FFN), D_MODEL ** -0.5).astype(jnp.bfloat16),
        "w_up": normal_scaled(base_keys[1], (NUM_LAYERS, D_MODEL, D_FFN), D_MODEL ** -0.5).astype(jnp.bfloat16),
        "w_down": normal_scaled(base_keys[2], (NUM_LAYERS, D_FFN, D_MODEL), D_FFN ** -0.5 * down_scale).astype(jnp.bfloat16),
        "norm_gain": (1.0 + normal_scaled(base_keys[3], (NUM_LAYERS, D_MODEL), 0.25)).astype(jnp.bfloat16),
        "a_up": normal_scaled(part_keys[0], (NUM_LAYERS, NUM_JOBS, D_MODEL, LORA_RANK), D_MODEL ** -0.5).astype(jnp.bfloat16),
        "b_up": normal_scaled(part_keys[1], (NUM_LAYERS, NUM_JOBS, LORA_RANK, D_FFN), 0.2 * LORA_RANK ** -0.5).astype(jnp.bfloat16),
        "a_down": normal_scaled(part_keys[2], (NUM_LAYERS, NUM_JOBS, D_FFN, LORA_RANK), D_FFN ** -0.5).astype(jnp.bfloat16),
        "b_down": normal_scaled(part_keys[3], (NUM_LAYERS, NUM_JOBS, LORA_RANK, D_MODEL), 0.2 * LORA_RANK ** -0.5 * down_scale).astype(jnp.bfloat16),
        "inputs": normal_scaled(part_keys[5], data_shape, 1.0).astype(jnp.bfloat16),
        "targets": normal_scaled(part_keys[6], data_shape, 1.0).astype(jnp.bfloat16),
        "lengths": lengths,
    }


def rms_norm(hidden, norm_gain):
    hidden_f32 = hidden.astype(jnp.float32)
    inv_rms = lax.rsqrt(jnp.mean(hidden_f32 * hidden_f32, axis=-1, keepdims=True) + NORM_EPS)
    return (hidden_f32 * inv_rms * norm_gain.astype(jnp.float32)).astype(jnp.bfloat16)


def mlp_layer(hidden, weights):
    w_gate, w_up, w_down, norm_gain, a_up, b_up, a_down, b_down = weights
    normed = rms_norm(hidden, norm_gain)
    gate_pre = jnp.dot(normed, w_gate, preferred_element_type=jnp.float32)
    low_up = jnp.dot(normed.astype(jnp.float32), a_up, preferred_element_type=jnp.float32).astype(jnp.bfloat16)
    up_val = jnp.dot(normed, w_up, preferred_element_type=jnp.float32) + LORA_SCALE * jnp.dot(low_up.astype(jnp.float32), b_up, preferred_element_type=jnp.float32)
    gated_prod = (jax.nn.silu(gate_pre) * up_val).astype(jnp.bfloat16)
    low_down = jnp.dot(gated_prod.astype(jnp.float32), a_down, preferred_element_type=jnp.float32).astype(jnp.bfloat16)
    layer_delta = jnp.dot(gated_prod, w_down, preferred_element_type=jnp.float32) + LORA_SCALE * jnp.dot(low_down.astype(jnp.float32), b_down, preferred_element_type=jnp.float32)
    return (hidden.astype(jnp.float32) + layer_delta).astype(jnp.bfloat16), None


def micro_loss(adapters, base_wts, x_micro, t_micro, len_micro, job_norm):
    hidden, _ = lax.scan(jax.checkpoint(mlp_layer), x_micro.reshape(TOKENS_MICRO, D_MODEL), base_wts + adapters)
    tok_mask = (jnp.arange(SEQ_LEN)[None, :] < len_micro[:, None]).astype(jnp.float32).reshape(TOKENS_MICRO, 1)
    residual = hidden.astype(jnp.float32) - t_micro.reshape(TOKENS_MICRO, D_MODEL).astype(jnp.float32)
    return 0.5 * jnp.sum(tok_mask * residual * residual) / job_norm


def reference(w_gate, w_up, w_down, norm_gain, a_up, b_up, a_down, b_down, inputs, targets, lengths):
    base_wts = (w_gate, w_up, w_down, norm_gain)
    job_norms = jnp.sum(lengths, axis=(1, 2)).astype(jnp.float32) * D_MODEL
    adapters_by_job = tuple(jnp.swapaxes(weight_arr, 0, 1).astype(jnp.float32) for weight_arr in (a_up, b_up, a_down, b_down))
    grad_fn = jax.value_and_grad(micro_loss)

    def job_fn(job_args):
        adapters, x_job, t_job, len_job, job_norm = job_args

        def micro_step(scan_carry, micro_args):
            loss_acc, grad_acc = scan_carry
            x_micro, t_micro, len_micro = micro_args
            loss_val, grads = grad_fn(adapters, base_wts, x_micro, t_micro, len_micro, job_norm)
            grad_acc = tuple(acc_arr + grad_val for acc_arr, grad_val in zip(grad_acc, grads))
            return (loss_acc + loss_val, grad_acc), None

        scan_init = (jnp.zeros((), jnp.float32), tuple(jnp.zeros_like(weight_arr) for weight_arr in adapters))
        (loss_total, grad_total), _ = lax.scan(micro_step, scan_init, (x_job, t_job, len_job))
        return loss_total, grad_total

    losses, grads = lax.map(job_fn, (adapters_by_job, inputs, targets, lengths, job_norms))
    grad_a_up, grad_b_up, grad_a_down, grad_b_down = grads
    return (losses, jnp.swapaxes(grad_a_up, 0, 1), jnp.swapaxes(grad_b_up, 0, 1), jnp.swapaxes(grad_a_down, 0, 1), jnp.swapaxes(grad_b_down, 0, 1))
```

```python
import functools

import jax
import jax.numpy as jnp
import numpy as np
from jax import lax
from jax.experimental import pallas as pl
from jax.experimental.pallas import tpu as pltpu
from jax.sharding import PartitionSpec as P

LORA_SCALE = 2.0
NORM_EPS = 1e-5
UNIT = 128
LANES = 256
FOLD = 128
PLANS = ((10,), (12,), (9, 9))
MESH_ID = pl.DeviceIdType.MESH
F32 = jnp.float32
BF16 = jnp.bfloat16


def dot_nn(lhs, rhs):
    return lax.dot_general(lhs, rhs, (((1,), (0,)), ((), ())), preferred_element_type=F32)


def dot_nt(lhs, rhs):
    return lax.dot_general(lhs, rhs, (((1,), (1,)), ((), ())), preferred_element_type=F32)


def dot_tn(lhs, rhs):
    return lax.dot_general(lhs, rhs, (((0,), (0,)), ((), ())), preferred_element_type=F32)


def fold(wide):
    return wide[:, :FOLD] + wide[:, FOLD:]


def unfold(folded, mask):
    return jnp.concatenate([folded, folded], axis=1) * mask


def sweep_kernel(units, stages,
                 w_gate, w_up, w_down, gain, a_up_hbm, b_up_hbm, a_down_hbm, b_down_hbm, rows_hbm, mask, weight,
                 loss_out, g_a_up, g_b_up, g_a_down, g_b_down,
                 h_in, g_in, gate_s, up_s, low_s, c_s, l_s, p_in, pl_in, s_in, sl_in, part, p_out, pl_out, s_out, sl_out, h_out, q_s, gup_s, gld_s, loss_in,
                 a_up, b_up, a_down, b_down, load_sem, adapter_sem, p_sem, pl_sem, s_sem, sl_sem, h_sem, g_sem, c_sem, l_sem, loss_sem,
                 p_send, pl_send, s_send, sl_send, h_send, c_send, l_send, g_send, loss_send):
    d_model = h_in.shape[2]
    used = g_a_up.shape[0]
    tp_idx = lax.axis_index("tp")
    stage = lax.axis_index("pp")
    last = stages - 1
    is_mid = lax.div(tp_idx + 1, 2) == 1
    is_end = lax.div(tp_idx + 1, 2) != 1
    mid_idx = 1 + lax.div(tp_idx, 2)
    end_idx = 3 * lax.div(tp_idx, 2)
    later = lax.rem(stage + 1, stages)
    earlier = lax.rem(stage + stages - 1, stages)
    cross_idx = 3 - tp_idx
    is_first = stage == 0
    is_last = stage == last

    def remote(src, dst, send, recv, tp_to, pp_to):
        return pltpu.make_async_remote_copy(src_ref=src, dst_ref=dst, send_sem=send, recv_sem=recv,
                                            device_id={"tp": tp_to, "pp": pp_to}, device_id_type=MESH_ID)

    load_inputs = pltpu.make_async_copy(rows_hbm, h_in, load_sem)
    load_targets = pltpu.make_async_copy(rows_hbm, g_in, load_sem)

    @pl.when(is_first)
    def _():
        load_inputs.start()

    @pl.when(is_last & is_mid)
    def _():
        load_targets.start()

    adapters = [(a_up_hbm, a_up), (b_up_hbm, b_up), (a_down_hbm, a_down), (b_down_hbm, b_down)]
    adapter_loads = [pltpu.make_async_copy(src, dst.at[pl.ds(0, used)], adapter_sem.at[which])
                     for which, (src, dst) in enumerate(adapters)]
    for load in adapter_loads:
        load.start()
    for _, dst in adapters:
        dst[pl.ds(used, LANES - used), :] = jnp.zeros((LANES - used, dst.shape[1]), BF16)

    barrier = pltpu.get_barrier_semaphore()

    def greet(tp_to, pp_to):
        pl.semaphore_signal(barrier, inc=1, device_id={"tp": tp_to, "pp": pp_to}, device_id_type=MESH_ID)

    @pl.when(is_mid)
    def _():
        greet(end_idx, stage)
        greet(cross_idx, stage)

        @pl.when(stage < last)
        def _():
            greet(mid_idx, later)
            greet(end_idx, later)

        @pl.when(stage > 0)
        def _():
            greet(mid_idx, earlier)
            greet(end_idx, earlier)

        pl.semaphore_wait(barrier, 2 + 2 * (stage < last).astype(jnp.int32) + 2 * (stage > 0).astype(jnp.int32))

    @pl.when(is_end)
    def _():
        greet(mid_idx, stage)

        @pl.when(stage < last)
        def _():
            greet(mid_idx, later)

        @pl.when(stage > 0)
        def _():
            greet(mid_idx, earlier)

        pl.semaphore_wait(barrier, 1 + (stage < last).astype(jnp.int32) + (stage > 0).astype(jnp.int32))

    loss_out[...] = jnp.zeros_like(loss_out)
    g_a_up[...] = jnp.zeros_like(g_a_up)
    g_b_up[...] = jnp.zeros_like(g_b_up)
    g_a_down[...] = jnp.zeros_like(g_a_down)
    g_b_down[...] = jnp.zeros_like(g_b_down)

    for load in adapter_loads:
        load.wait()

    @pl.when(is_first)
    def _():
        load_inputs.wait()

    @pl.when(is_last & is_mid)
    def _():
        load_targets.wait()

    def part_copy(idx, slot):
        return remote(p_out.at[slot], p_in.at[idx], p_send.at[slot], p_sem.at[idx], mid_idx, stage)

    def part_low_copy(idx, slot):
        return remote(pl_out.at[slot], pl_in.at[idx], pl_send.at[slot], pl_sem.at[idx], mid_idx, stage)

    def sum_copy(idx, slot):
        land = 2 * idx + lax.div(slot, 2)
        return remote(s_out.at[slot], s_in.at[land], s_send.at[slot], s_sem.at[land], cross_idx, stage)

    def sum_low_copy(idx, slot):
        land = 2 * idx + lax.div(slot, 2)
        return remote(sl_out.at[slot], sl_in.at[land], sl_send.at[slot], sl_sem.at[land], cross_idx, stage)

    def hidden_copy(idx, slot, which):
        return remote(h_out.at[slot], h_in.at[idx], h_send.at[slot, which], h_sem.at[idx],
                      (mid_idx, end_idx)[which], later)

    def grad_copy(idx, slot, which):
        return remote(h_out.at[slot], g_in.at[idx], h_send.at[slot, which], g_sem.at[idx],
                      (mid_idx, end_idx)[which], earlier)

    def top_copy(idx):
        return remote(g_in.at[idx], g_in.at[idx], g_send.at[idx], g_sem.at[idx], end_idx, stage)

    def c_copy(idx):
        return remote(c_s.at[idx], c_s.at[idx], c_send.at[idx], c_sem.at[idx], end_idx, stage)

    def l_copy(idx):
        return remote(l_s.at[idx], l_s.at[idx], l_send.at[idx], l_sem.at[idx], end_idx, stage)

    def loss_copy(which):
        return remote(loss_out, loss_in, loss_send.at[which], loss_sem,
                      (mid_idx, end_idx)[which], earlier)

    def loss_copy_same():
        return remote(loss_out, loss_in, loss_send.at[2], loss_sem, end_idx, stage)

    def normed_of(hidden_f32):
        inv_rms = lax.rsqrt(jnp.mean(hidden_f32 * hidden_f32, axis=-1, keepdims=True) + NORM_EPS)
        return inv_rms, (hidden_f32 * inv_rms * gain[...]).astype(BF16)

    def at(unit):
        return jnp.clip(unit, 0, units - 1)

    def fwd_iter(step, carry):
        @pl.when(step < units)
        def _():
            idx = at(step)
            slot = lax.rem(idx, 2)

            @pl.when(stage > 0)
            def _():
                hidden_copy(idx, slot, 0).wait_recv()

            _, normed = normed_of(h_in[idx].astype(F32))
            mask_rows = mask[idx]
            low = dot_nt(normed, a_up[...]).astype(BF16) * mask_rows
            low_s[idx] = low
            gate_pre = dot_nt(normed, w_gate[...])
            gate_s[idx] = gate_pre
            up_val = dot_nt(normed, w_up[...]) + LORA_SCALE * dot_nn(low, b_up[...])
            up_s[idx] = up_val
            prod = (gate_pre * jax.nn.sigmoid(gate_pre) * up_val).astype(BF16)
            down = dot_nn(prod, w_down[...])
            low_down = fold(dot_nt(prod, a_down[...]) * mask_rows.astype(F32))

            @pl.when(is_mid)
            def _():
                part[slot, :, pl.ds(0, d_model)] = down
                part[slot, :, pl.ds(d_model, FOLD)] = low_down

            @pl.when(is_end)
            def _():
                @pl.when(idx >= 2)
                def _():
                    part_copy(at(idx - 2), slot).wait_send()
                    part_low_copy(at(idx - 2), slot).wait_send()

                p_out[slot] = down.astype(BF16)
                part_copy(idx, slot).start()
                pl_out[slot] = low_down.astype(BF16)
                part_low_copy(idx, slot).start()

        @pl.when(is_mid & (step >= 1) & (step <= units))
        def _():
            unit = at(step - 1)
            slot = lax.rem(unit, 2)
            part_copy(unit, slot).wait_recv()
            part_low_copy(unit, slot).wait_recv()

            @pl.when(unit >= 2)
            def _():
                sum_copy(at(unit - 2), slot).wait_send()
                sum_low_copy(at(unit - 2), slot).wait_send()

            s_out[slot] = (part[slot, :, pl.ds(0, d_model)] + p_in[unit].astype(F32)).astype(BF16)
            sum_copy(unit, slot).start()
            sl_out[slot] = (part[slot, :, pl.ds(d_model, FOLD)] + pl_in[unit].astype(F32)).astype(BF16)
            sum_low_copy(unit, slot).start()

        @pl.when(is_mid & (step >= 2))
        def _():
            unit = at(step - 2)
            slot = lax.rem(unit, 2)
            sum_copy(unit, slot).wait_recv()
            sum_low_copy(unit, slot).wait_recv()
            total = s_out[slot].astype(F32) + s_in[2 * unit].astype(F32)
            c_fold = (sl_out[slot].astype(F32) + sl_in[2 * unit].astype(F32)).astype(BF16)
            c_s[unit] = c_fold
            c_copy(unit).start()
            mask_rows = mask[unit]
            delta = total + LORA_SCALE * dot_nn(unfold(c_fold, mask_rows), b_down[...])
            hidden = (h_in[unit].astype(F32) + delta).astype(BF16)

            @pl.when(stage < last)
            def _():
                @pl.when(unit >= 2)
                def _():
                    hidden_copy(at(unit - 2), slot, 0).wait_send()
                    hidden_copy(at(unit - 2), slot, 1).wait_send()

                h_out[slot] = hidden
                hidden_copy(unit, slot, 0).start()
                hidden_copy(unit, slot, 1).start()

            @pl.when(is_last)
            def _():
                residual = hidden.astype(F32) - g_in[unit].astype(F32)
                weighted = weight[unit][:, :1] * residual
                g_in[unit] = weighted.astype(BF16)
                top_copy(unit).start()
                row_sum = jnp.sum(weighted * residual, axis=-1, keepdims=True)
                loss_out[...] += jnp.broadcast_to(
                    jnp.sum(row_sum * mask_rows.astype(F32), axis=0, keepdims=True), loss_out.shape)

        return carry

    lax.fori_loop(0, units + 2, fwd_iter, 0)

    def bwd_iter(step, carry):
        @pl.when(step < units)
        def _():
            idx = at(step)
            slot = lax.rem(idx, 2)

            @pl.when(jnp.logical_not(is_last & is_mid))
            def _():
                grad_copy(idx, slot + 2, 0).wait_recv()

            grad = g_in[idx]
            mask_rows = mask[idx]
            g_low = (LORA_SCALE * dot_nt(grad, b_down[...])).astype(BF16) * mask_rows
            gld_s[...] = g_low
            g_prod = dot_nt(grad, w_down[...]) + dot_nn(g_low, a_down[...])
            gate_pre = gate_s[idx]
            up_val = up_s[idx]
            sig = jax.nn.sigmoid(gate_pre)
            act = gate_pre * sig
            q_s[...] = (act * up_val).astype(BF16)
            g_up = (g_prod * act).astype(BF16)
            gup_s[...] = g_up
            g_gate = (g_prod * up_val * (sig * (1.0 + gate_pre * (1.0 - sig)))).astype(BF16)
            g_low_up = fold(dot_nt(g_up, b_up[...]) * mask_rows.astype(F32))

            @pl.when(is_mid)
            def _():
                part[slot, :, pl.ds(d_model, FOLD)] = g_low_up

            @pl.when(is_end)
            def _():
                @pl.when(idx >= 2)
                def _():
                    part_low_copy(at(idx - 2), slot + 2).wait_send()

                pl_out[slot + 2] = g_low_up.astype(BF16)
                part_low_copy(idx, slot + 2).start()

            @pl.when(stage > 0)
            def _():
                g_norm = dot_nn(g_gate, w_gate[...]) + dot_nn(g_up, w_up[...])

                @pl.when(is_mid)
                def _():
                    part[slot, :, pl.ds(0, d_model)] = g_norm

                @pl.when(is_end)
                def _():
                    @pl.when(idx >= 2)
                    def _():
                        part_copy(at(idx - 2), slot + 2).wait_send()

                    p_out[slot + 2] = g_norm.astype(BF16)
                    part_copy(idx, slot + 2).start()

        @pl.when(is_mid & (step >= 1) & (step <= units))
        def _():
            unit = at(step - 1)
            slot = lax.rem(unit, 2)
            part_low_copy(unit, slot + 2).wait_recv()

            @pl.when(unit >= 2)
            def _():
                sum_low_copy(at(unit - 2), slot + 2).wait_send()

            sl_out[slot + 2] = (part[slot, :, pl.ds(d_model, FOLD)] + pl_in[unit].astype(F32)).astype(BF16)
            sum_low_copy(unit, slot + 2).start()

            @pl.when(stage > 0)
            def _():
                part_copy(unit, slot + 2).wait_recv()

                @pl.when(unit >= 2)
                def _():
                    sum_copy(at(unit - 2), slot + 2).wait_send()

                s_out[slot + 2] = (part[slot, :, pl.ds(0, d_model)] + p_in[unit].astype(F32)).astype(BF16)
                sum_copy(unit, slot + 2).start()

        @pl.when(is_mid & (step >= 2) & (step <= units + 1))
        def _():
            unit = at(step - 2)
            slot = lax.rem(unit, 2)
            sum_low_copy(unit, slot + 2).wait_recv()
            low_total = sl_out[slot + 2].astype(F32) + sl_in[2 * unit + 1].astype(F32)
            l_fold = (LORA_SCALE * low_total).astype(BF16)
            l_s[unit] = l_fold
            l_copy(unit).start()

            @pl.when(stage > 0)
            def _():
                sum_copy(unit, slot + 2).wait_recv()
                total = s_out[slot + 2].astype(F32) + s_in[2 * unit + 1].astype(F32)
                g_normed = total + dot_nn(unfold(l_fold, mask[unit]), a_up[...])
                hidden_f32 = h_in[unit].astype(F32)
                inv_rms = lax.rsqrt(jnp.mean(hidden_f32 * hidden_f32, axis=-1, keepdims=True) + NORM_EPS)
                g_scaled = g_normed * gain[...]
                unit_rows = hidden_f32 * inv_rms
                g_hidden = inv_rms * (g_scaled - unit_rows * jnp.mean(g_scaled * unit_rows, axis=-1, keepdims=True))

                @pl.when(unit >= 2)
                def _():
                    grad_copy(at(unit - 2), slot + 2, 0).wait_send()
                    grad_copy(at(unit - 2), slot + 2, 1).wait_send()

                h_out[slot + 2] = (g_in[unit].astype(F32) + g_hidden).astype(BF16)
                grad_copy(unit, slot + 2, 0).start()
                grad_copy(unit, slot + 2, 1).start()

        @pl.when(step < units)
        def _():
            idx = at(step)

            @pl.when(is_end)
            def _():
                c_copy(idx).wait_recv()

            mask_rows = mask[idx]
            g_low = gld_s[...]
            g_a_down[...] += dot_tn(g_low, q_s[...])[:used]
            g_b_up[...] += dot_tn(low_s[idx], gup_s[...])[:used]
            g_b_down[...] += dot_tn(unfold(c_s[idx], mask_rows), g_in[idx])[:used]

        @pl.when(step >= 3)
        def _():
            unit = at(step - 3)

            @pl.when(is_end)
            def _():
                l_copy(unit).wait_recv()

            _, normed = normed_of(h_in[unit].astype(F32))
            g_a_up[...] += dot_tn(unfold(l_s[unit], mask[unit]), normed)[:used]

        return carry

    lax.fori_loop(0, units + 3, bwd_iter, 0)
    g_b_up[...] = LORA_SCALE * g_b_up[...]
    g_b_down[...] = LORA_SCALE * g_b_down[...]

    @pl.when(is_mid & is_last)
    def _():
        loss_copy_same().start()

    @pl.when(jnp.logical_not(is_mid & is_last))
    def _():
        loss_copy(0).wait_recv()
        loss_out[...] = loss_in[...]

    @pl.when(is_mid & (stage > 0))
    def _():
        loss_copy(0).start()
        loss_copy(1).start()

    @pl.when(is_mid & is_last)
    def _():
        loss_copy_same().wait_send()

    @pl.when(is_mid & (stage > 0))
    def _():
        loss_copy(0).wait_send()
        loss_copy(1).wait_send()

    for unit in (units - 2, units - 1):
        slot = jnp.int32(unit % 2)

        @pl.when(is_end)
        def _():
            part_copy(unit, slot).wait_send()
            part_low_copy(unit, slot).wait_send()
            part_low_copy(unit, slot + 2).wait_send()

            @pl.when(stage > 0)
            def _():
                part_copy(unit, slot + 2).wait_send()

        @pl.when(is_mid)
        def _():
            sum_copy(unit, slot).wait_send()
            sum_low_copy(unit, slot).wait_send()
            sum_low_copy(unit, slot + 2).wait_send()

            @pl.when(stage < last)
            def _():
                hidden_copy(unit, slot, 0).wait_send()
                hidden_copy(unit, slot, 1).wait_send()

            @pl.when(stage > 0)
            def _():
                sum_copy(unit, slot + 2).wait_send()
                grad_copy(unit, slot + 2, 0).wait_send()
                grad_copy(unit, slot + 2, 1).wait_send()

    @pl.when(is_mid)
    def _():
        def drain(idx, carry):
            c_copy(idx).wait_send()
            l_copy(idx).wait_send()

            @pl.when(is_last)
            def _():
                top_copy(idx).wait_send()

            return carry

        lax.fori_loop(0, units, drain, 0)


def sweep(units, stages, weights, rows, mask, weight, collective_id):
    width, d_model = weights[0].shape
    used = weights[4].shape[0]
    msg = d_model + FOLD
    vmem = pl.BlockSpec(memory_space=pltpu.VMEM)
    out_shape = (
        jax.ShapeDtypeStruct((8, LANES), F32),
        jax.ShapeDtypeStruct((used, d_model), F32),
        jax.ShapeDtypeStruct((used, width), F32),
        jax.ShapeDtypeStruct((used, width), F32),
        jax.ShapeDtypeStruct((used, d_model), F32),
    )
    dma = pltpu.SemaphoreType.DMA
    return pl.pallas_call(
        functools.partial(sweep_kernel, units, stages),
        out_shape=out_shape,
        in_specs=[vmem] * 4 + [pl.BlockSpec(memory_space=pltpu.HBM)] * 5 + [vmem] * 2,
        out_specs=(vmem,) * 5,
        scratch_shapes=[
            pltpu.VMEM((units, UNIT, d_model), BF16),
            pltpu.VMEM((units, UNIT, d_model), BF16),
            pltpu.VMEM((units, UNIT, width), F32),
            pltpu.VMEM((units, UNIT, width), F32),
            pltpu.VMEM((units, UNIT, LANES), BF16),
            pltpu.VMEM((units, UNIT, FOLD), BF16),
            pltpu.VMEM((units, UNIT, FOLD), BF16),
            pltpu.VMEM((units, UNIT, d_model), BF16),
            pltpu.VMEM((units, UNIT, FOLD), BF16),
            pltpu.VMEM((2 * units, UNIT, d_model), BF16),
            pltpu.VMEM((2 * units, UNIT, FOLD), BF16),
            pltpu.VMEM((2, UNIT, msg), F32),
            pltpu.VMEM((4, UNIT, d_model), BF16),
            pltpu.VMEM((4, UNIT, FOLD), BF16),
            pltpu.VMEM((4, UNIT, d_model), BF16),
            pltpu.VMEM((4, UNIT, FOLD), BF16),
            pltpu.VMEM((4, UNIT, d_model), BF16),
            pltpu.VMEM((UNIT, width), BF16),
            pltpu.VMEM((UNIT, width), BF16),
            pltpu.VMEM((UNIT, LANES), BF16),
            pltpu.VMEM((8, LANES), F32),
            pltpu.VMEM((LANES, d_model), BF16),
            pltpu.VMEM((LANES, width), BF16),
            pltpu.VMEM((LANES, width), BF16),
            pltpu.VMEM((LANES, d_model), BF16),
            dma,
            dma((4,)),
            dma((units,)),
            dma((units,)),
            dma((2 * units,)),
            dma((2 * units,)),
            dma((units,)),
            dma((units,)),
            dma((units,)),
            dma((units,)),
            dma,
            dma((4,)),
            dma((4,)),
            dma((4,)),
            dma((4,)),
            dma((4, 2)),
            dma((units,)),
            dma((units,)),
            dma((units,)),
            dma((3,)),
        ],
        compiler_params=pltpu.CompilerParams(collective_id=collective_id, has_side_effects=True,
                                             vmem_limit_bytes=66_000_000),
    )(*weights, rows, mask, weight)


def solution(mesh):
    num_stages = mesh.shape["pp"]

    def stage_body(w_gate, w_up, w_down, norm_gain, a_up, b_up, a_down, b_down, inputs, targets, lengths):
        stage_idx = lax.axis_index("pp")
        num_jobs, num_micro, row_count, seq_len, d_model = inputs.shape
        rank = a_up.shape[-1]
        job_rows = num_micro * row_count
        num_rows = num_jobs * job_rows
        num_tokens = num_rows * seq_len
        width = w_gate.shape[-1]
        used = num_jobs * rank

        order = np.arange(num_rows).reshape(lengths.shape)
        row_lens = jnp.sum(jnp.where(np.arange(num_rows)[:, None, None, None] == order[None], lengths[None], 0), axis=(1, 2, 3))
        row_ends = jnp.cumsum(row_lens)
        row_starts = row_ends - row_lens
        job_norms = jnp.sum(lengths, axis=(1, 2)).astype(F32) * d_model
        row_jobs = jnp.arange(num_rows) // job_rows
        row_shift = jnp.arange(num_rows) * seq_len - row_starts
        row_weight = jnp.repeat(1.0 / job_norms, job_rows)

        a_up_all = jnp.swapaxes(a_up[0], 1, 2).reshape(used, d_model)
        b_up_all = b_up[0].reshape(used, width)
        a_down_all = jnp.swapaxes(a_down[0], 1, 2).reshape(used, width)
        b_down_all = b_down[0].reshape(used, d_model)
        gain = jnp.broadcast_to(norm_gain.astype(F32), (UNIT, d_model))
        weights = (jnp.swapaxes(w_gate[0], 0, 1), jnp.swapaxes(w_up[0], 0, 1), w_down[0], gain, a_up_all, b_up_all, a_down_all, b_down_all)
        rows_all = jnp.where(stage_idx == num_stages - 1, targets, inputs).reshape(num_tokens, d_model)

        def run(plan):
            def one_pass(units, first):
                slots = first + jnp.arange(units * UNIT)
                in_row = (slots[:, None] >= row_starts[None, :]) & (slots[:, None] < row_ends[None, :])
                valid = slots < row_ends[-1]
                source = slots + jnp.sum(jnp.where(in_row, row_shift[None, :], 0), axis=1)
                job = jnp.sum(jnp.where(in_row, row_jobs[None, :], 0), axis=1)
                weight = jnp.sum(jnp.where(in_row, row_weight[None, :], 0.0), axis=1)
                pick = ((source[:, None] == jnp.arange(num_tokens)[None, :]) & valid[:, None]).astype(BF16)
                rows = jnp.dot(pick, rows_all, preferred_element_type=F32).astype(BF16)
                mask = ((jnp.arange(LANES)[None, :] // rank == job[:, None]) & valid[:, None]).astype(BF16)
                return sweep(units, num_stages, weights,
                             rows.reshape(units, UNIT, d_model), mask.reshape(units, UNIT, LANES),
                             jnp.broadcast_to(weight[:, None], (units * UNIT, FOLD)).reshape(units, UNIT, FOLD), 0)

            if len(plan) == 1:
                return tuple(one_pass(plan[0], 0))
            zeros = tuple(jnp.zeros(shape, F32) for shape in ((8, LANES), (used, d_model), (used, width), (used, width), (used, d_model)))
            return lax.fori_loop(0, len(plan), lambda turn, outs: tuple(
                old + add for old, add in zip(outs, one_pass(plan[0], turn * plan[0] * UNIT))), zeros)

        caps = [sum(plan) * UNIT for plan in PLANS]
        choice = sum((row_ends[-1] > cap).astype(jnp.int32) for cap in caps[:-1])
        loss, g_a_up, g_b_up, g_a_down, g_b_down = lax.switch(choice, [functools.partial(run, plan) for plan in PLANS])
        losses = 0.5 * loss[0, :used:rank]
        g_a_up = jnp.swapaxes(g_a_up.reshape(1, num_jobs, rank, d_model), 2, 3)
        g_b_up = g_b_up.reshape(1, num_jobs, rank, width)
        g_a_down = jnp.swapaxes(g_a_down.reshape(1, num_jobs, rank, width), 2, 3)
        g_b_down = g_b_down.reshape(1, num_jobs, rank, d_model)
        return losses, g_a_up, g_b_up, g_a_down, g_b_down

    weight_specs = (P("pp", None, "tp"), P("pp", None, "tp"), P("pp", "tp", None), P("pp", None))
    adapter_specs = (P("pp", "rep", None, None), P("pp", "rep", None, "tp"), P("pp", "rep", "tp", None), P("pp", "rep", None, None))
    data_specs = (P("rep"), P("rep"), P("rep"))
    return jax.shard_map(stage_body, mesh=mesh, in_specs=weight_specs + adapter_specs + data_specs,
                         out_specs=(P("rep"),) + adapter_specs, check_vma=False)
```

```python
import functools

import jax
import jax.numpy as jnp
import numpy as np
from jax import lax
from jax.experimental import pallas as pl
from jax.experimental.pallas import tpu as pltpu
from jax.sharding import PartitionSpec as P

LORA_SCALE = 2.0
NORM_EPS = 1e-5
UNIT = 128
LANES = 256
FOLD = 128
PLANS = ((10,), (12,), (9, 9))
MESH_ID = pl.DeviceIdType.MESH
F32 = jnp.float32
BF16 = jnp.bfloat16


def dot_nn(lhs, rhs):
    return lax.dot_general(lhs, rhs, (((1,), (0,)), ((), ())), preferred_element_type=F32)


def dot_nt(lhs, rhs):
    return lax.dot_general(lhs, rhs, (((1,), (1,)), ((), ())), preferred_element_type=F32)


def dot_tn(lhs, rhs):
    return lax.dot_general(lhs, rhs, (((0,), (0,)), ((), ())), preferred_element_type=F32)


def fold(wide):
    return wide[:, :FOLD] + wide[:, FOLD:]


def unfold(folded, mask):
    return jnp.concatenate([folded, folded], axis=1) * mask


def sweep_kernel(units, stages,
                 w_gate, w_up, w_down, gain, a_up_hbm, b_up_hbm, a_down_hbm, b_down_hbm, rows_hbm, mask, weight,
                 loss_out, g_a_up, g_b_up, g_a_down, g_b_down,
                 h_in, g_in, gate_s, up_s, low_s, c_s, l_s, p_in, pl_in, s_in, sl_in, part, p_out, pl_out, s_out, sl_out, h_out, q_s, gup_s, gld_s, loss_in,
                 a_up, b_up, a_down, b_down, load_sem, adapter_sem, p_sem, pl_sem, s_sem, sl_sem, h_sem, g_sem, c_sem, l_sem, loss_sem,
                 p_send, pl_send, s_send, sl_send, h_send, c_send, l_send, g_send, loss_send):
    d_model = h_in.shape[2]
    used = g_a_up.shape[0]
    tp_idx = lax.axis_index("tp")
    stage = lax.axis_index("pp")
    last = stages - 1
    is_mid = lax.div(tp_idx + 1, 2) == 1
    is_end = lax.div(tp_idx + 1, 2) != 1
    mid_idx = 1 + lax.div(tp_idx, 2)
    end_idx = 3 * lax.div(tp_idx, 2)
    later = lax.rem(stage + 1, stages)
    earlier = lax.rem(stage + stages - 1, stages)
    cross_idx = 3 - tp_idx
    is_first = stage == 0
    is_last = stage == last

    def remote(src, dst, send, recv, tp_to, pp_to):
        return pltpu.make_async_remote_copy(src_ref=src, dst_ref=dst, send_sem=send, recv_sem=recv,
                                            device_id={"tp": tp_to, "pp": pp_to}, device_id_type=MESH_ID)

    load_inputs = pltpu.make_async_copy(rows_hbm, h_in, load_sem)
    load_targets = pltpu.make_async_copy(rows_hbm, g_in, load_sem)

    @pl.when(is_first)
    def _():
        load_inputs.start()

    @pl.when(is_last & is_mid)
    def _():
        load_targets.start()

    adapters = [(a_up_hbm, a_up), (b_up_hbm, b_up), (a_down_hbm, a_down), (b_down_hbm, b_down)]
    adapter_loads = [pltpu.make_async_copy(src, dst.at[pl.ds(0, used)], adapter_sem.at[which])
                     for which, (src, dst) in enumerate(adapters)]
    for load in adapter_loads:
        load.start()
    for _, dst in adapters:
        dst[pl.ds(used, LANES - used), :] = jnp.zeros((LANES - used, dst.shape[1]), BF16)

    barrier = pltpu.get_barrier_semaphore()

    def greet(tp_to, pp_to):
        pl.semaphore_signal(barrier, inc=1, device_id={"tp": tp_to, "pp": pp_to}, device_id_type=MESH_ID)

    @pl.when(is_mid)
    def _():
        greet(end_idx, stage)
        greet(cross_idx, stage)

        @pl.when(stage < last)
        def _():
            greet(mid_idx, later)
            greet(end_idx, later)

        @pl.when(stage > 0)
        def _():
            greet(mid_idx, earlier)
            greet(end_idx, earlier)

        pl.semaphore_wait(barrier, 2 + 2 * (stage < last).astype(jnp.int32) + 2 * (stage > 0).astype(jnp.int32))

    @pl.when(is_end)
    def _():
        greet(mid_idx, stage)

        @pl.when(stage < last)
        def _():
            greet(mid_idx, later)

        @pl.when(stage > 0)
        def _():
            greet(mid_idx, earlier)

        pl.semaphore_wait(barrier, 1 + (stage < last).astype(jnp.int32) + (stage > 0).astype(jnp.int32))

    loss_out[...] = jnp.zeros_like(loss_out)
    g_a_up[...] = jnp.zeros_like(g_a_up)
    g_b_up[...] = jnp.zeros_like(g_b_up)
    g_a_down[...] = jnp.zeros_like(g_a_down)
    g_b_down[...] = jnp.zeros_like(g_b_down)

    for load in adapter_loads:
        load.wait()

    @pl.when(is_first)
    def _():
        load_inputs.wait()

    @pl.when(is_last & is_mid)
    def _():
        load_targets.wait()

    def part_copy(idx, slot):
        return remote(p_out.at[slot], p_in.at[idx], p_send.at[slot], p_sem.at[idx], mid_idx, stage)

    def part_low_copy(idx, slot):
        return remote(pl_out.at[slot], pl_in.at[idx], pl_send.at[slot], pl_sem.at[idx], mid_idx, stage)

    def sum_copy(idx, slot):
        land = 2 * idx + lax.div(slot, 2)
        return remote(s_out.at[slot], s_in.at[land], s_send.at[slot], s_sem.at[land], cross_idx, stage)

    def sum_low_copy(idx, slot):
        land = 2 * idx + lax.div(slot, 2)
        return remote(sl_out.at[slot], sl_in.at[land], sl_send.at[slot], sl_sem.at[land], cross_idx, stage)

    def hidden_copy(idx, slot, which):
        return remote(h_out.at[slot], h_in.at[idx], h_send.at[slot, which], h_sem.at[idx],
                      (mid_idx, end_idx)[which], later)

    def grad_copy(idx, slot, which):
        return remote(h_out.at[slot], g_in.at[idx], h_send.at[slot, which], g_sem.at[idx],
                      (mid_idx, end_idx)[which], earlier)

    def top_copy(idx):
        return remote(g_in.at[idx], g_in.at[idx], g_send.at[idx], g_sem.at[idx], end_idx, stage)

    def c_copy(idx):
        return remote(c_s.at[idx], c_s.at[idx], c_send.at[idx], c_sem.at[idx], end_idx, stage)

    def l_copy(idx):
        return remote(l_s.at[idx], l_s.at[idx], l_send.at[idx], l_sem.at[idx], end_idx, stage)

    def loss_copy(which):
        return remote(loss_out, loss_in, loss_send.at[which], loss_sem,
                      (mid_idx, end_idx)[which], earlier)

    def loss_copy_same():
        return remote(loss_out, loss_in, loss_send.at[2], loss_sem, end_idx, stage)

    def normed_of(hidden_f32):
        inv_rms = lax.rsqrt(jnp.mean(hidden_f32 * hidden_f32, axis=-1, keepdims=True) + NORM_EPS)
        return inv_rms, (hidden_f32 * inv_rms * gain[...]).astype(BF16)

    def at(unit):
        return jnp.clip(unit, 0, units - 1)

    def fwd_iter(step, carry):
        @pl.when(is_mid & (step >= 2))
        def _():
            unit = at(step - 2)
            slot = lax.rem(unit, 2)
            sum_copy(unit, slot).wait_recv()
            sum_low_copy(unit, slot).wait_recv()
            total = s_out[slot].astype(F32) + s_in[2 * unit].astype(F32)
            c_fold = (sl_out[slot].astype(F32) + sl_in[2 * unit].astype(F32)).astype(BF16)
            c_s[unit] = c_fold
            c_copy(unit).start()
            mask_rows = mask[unit]
            delta = total + LORA_SCALE * dot_nn(unfold(c_fold, mask_rows), b_down[...])
            hidden = (h_in[unit].astype(F32) + delta).astype(BF16)

            @pl.when(stage < last)
            def _():
                @pl.when(unit >= 2)
                def _():
                    hidden_copy(at(unit - 2), slot, 0).wait_send()
                    hidden_copy(at(unit - 2), slot, 1).wait_send()

                h_out[slot] = hidden
                hidden_copy(unit, slot, 0).start()
                hidden_copy(unit, slot, 1).start()

            @pl.when(is_last)
            def _():
                residual = hidden.astype(F32) - g_in[unit].astype(F32)
                weighted = weight[unit][:, :1] * residual
                g_in[unit] = weighted.astype(BF16)
                top_copy(unit).start()
                row_sum = jnp.sum(weighted * residual, axis=-1, keepdims=True)
                loss_out[...] += jnp.broadcast_to(
                    jnp.sum(row_sum * mask_rows.astype(F32), axis=0, keepdims=True), loss_out.shape)

        @pl.when(is_mid & (step >= 1) & (step <= units))
        def _():
            unit = at(step - 1)
            slot = lax.rem(unit, 2)
            part_copy(unit, slot).wait_recv()
            part_low_copy(unit, slot).wait_recv()

            @pl.when(unit >= 2)
            def _():
                sum_copy(at(unit - 2), slot).wait_send()
                sum_low_copy(at(unit - 2), slot).wait_send()

            s_out[slot] = (part[slot, :, pl.ds(0, d_model)] + p_in[unit].astype(F32)).astype(BF16)
            sum_copy(unit, slot).start()
            sl_out[slot] = (part[slot, :, pl.ds(d_model, FOLD)] + pl_in[unit].astype(F32)).astype(BF16)
            sum_low_copy(unit, slot).start()

        @pl.when(step < units)
        def _():
            idx = at(step)
            slot = lax.rem(idx, 2)

            @pl.when(stage > 0)
            def _():
                hidden_copy(idx, slot, 0).wait_recv()

            _, normed = normed_of(h_in[idx].astype(F32))
            mask_rows = mask[idx]
            low = dot_nt(normed, a_up[...]).astype(BF16) * mask_rows
            low_s[idx] = low
            gate_pre = dot_nt(normed, w_gate[...])
            gate_s[idx] = gate_pre
            up_val = dot_nt(normed, w_up[...]) + LORA_SCALE * dot_nn(low, b_up[...])
            up_s[idx] = up_val
            prod = (gate_pre * jax.nn.sigmoid(gate_pre) * up_val).astype(BF16)
            down = dot_nn(prod, w_down[...])
            low_down = fold(dot_nt(prod, a_down[...]) * mask_rows.astype(F32))

            @pl.when(is_mid)
            def _():
                part[slot, :, pl.ds(0, d_model)] = down
                part[slot, :, pl.ds(d_model, FOLD)] = low_down

            @pl.when(is_end)
            def _():
                @pl.when(idx >= 2)
                def _():
                    part_copy(at(idx - 2), slot).wait_send()
                    part_low_copy(at(idx - 2), slot).wait_send()

                p_out[slot] = down.astype(BF16)
                part_copy(idx, slot).start()
                pl_out[slot] = low_down.astype(BF16)
                part_low_copy(idx, slot).start()

        return carry

    lax.fori_loop(0, units + 2, fwd_iter, 0)

    def bwd_iter(step, carry):
        @pl.when(is_mid & (step >= 2) & (step <= units + 1))
        def _():
            unit = at(step - 2)
            slot = lax.rem(unit, 2)
            sum_low_copy(unit, slot + 2).wait_recv()
            low_total = sl_out[slot + 2].astype(F32) + sl_in[2 * unit + 1].astype(F32)
            l_fold = (LORA_SCALE * low_total).astype(BF16)
            l_s[unit] = l_fold
            l_copy(unit).start()

            @pl.when(stage > 0)
            def _():
                sum_copy(unit, slot + 2).wait_recv()
                total = s_out[slot + 2].astype(F32) + s_in[2 * unit + 1].astype(F32)
                g_normed = total + dot_nn(unfold(l_fold, mask[unit]), a_up[...])
                hidden_f32 = h_in[unit].astype(F32)
                inv_rms = lax.rsqrt(jnp.mean(hidden_f32 * hidden_f32, axis=-1, keepdims=True) + NORM_EPS)
                g_scaled = g_normed * gain[...]
                unit_rows = hidden_f32 * inv_rms
                g_hidden = inv_rms * (g_scaled - unit_rows * jnp.mean(g_scaled * unit_rows, axis=-1, keepdims=True))

                @pl.when(unit >= 2)
                def _():
                    grad_copy(at(unit - 2), slot + 2, 0).wait_send()
                    grad_copy(at(unit - 2), slot + 2, 1).wait_send()

                h_out[slot + 2] = (g_in[unit].astype(F32) + g_hidden).astype(BF16)
                grad_copy(unit, slot + 2, 0).start()
                grad_copy(unit, slot + 2, 1).start()

        @pl.when(is_mid & (step >= 1) & (step <= units))
        def _():
            unit = at(step - 1)
            slot = lax.rem(unit, 2)
            part_low_copy(unit, slot + 2).wait_recv()

            @pl.when(unit >= 2)
            def _():
                sum_low_copy(at(unit - 2), slot + 2).wait_send()

            sl_out[slot + 2] = (part[slot, :, pl.ds(d_model, FOLD)] + pl_in[unit].astype(F32)).astype(BF16)
            sum_low_copy(unit, slot + 2).start()

            @pl.when(stage > 0)
            def _():
                part_copy(unit, slot + 2).wait_recv()

                @pl.when(unit >= 2)
                def _():
                    sum_copy(at(unit - 2), slot + 2).wait_send()

                s_out[slot + 2] = (part[slot, :, pl.ds(0, d_model)] + p_in[unit].astype(F32)).astype(BF16)
                sum_copy(unit, slot + 2).start()

        @pl.when(step < units)
        def _():
            idx = at(step)
            slot = lax.rem(idx, 2)

            @pl.when(jnp.logical_not(is_last & is_mid))
            def _():
                grad_copy(idx, slot + 2, 0).wait_recv()

            grad = g_in[idx]
            mask_rows = mask[idx]
            g_low = (LORA_SCALE * dot_nt(grad, b_down[...])).astype(BF16) * mask_rows
            gld_s[...] = g_low
            g_prod = dot_nt(grad, w_down[...]) + dot_nn(g_low, a_down[...])
            gate_pre = gate_s[idx]
            up_val = up_s[idx]
            sig = jax.nn.sigmoid(gate_pre)
            act = gate_pre * sig
            q_s[...] = (act * up_val).astype(BF16)
            g_up = (g_prod * act).astype(BF16)
            gup_s[...] = g_up
            g_gate = (g_prod * up_val * (sig * (1.0 + gate_pre * (1.0 - sig)))).astype(BF16)
            g_low_up = fold(dot_nt(g_up, b_up[...]) * mask_rows.astype(F32))

            @pl.when(is_mid)
            def _():
                part[slot, :, pl.ds(d_model, FOLD)] = g_low_up

            @pl.when(is_end)
            def _():
                @pl.when(idx >= 2)
                def _():
                    part_low_copy(at(idx - 2), slot + 2).wait_send()

                pl_out[slot + 2] = g_low_up.astype(BF16)
                part_low_copy(idx, slot + 2).start()

            @pl.when(stage > 0)
            def _():
                g_norm = dot_nn(g_gate, w_gate[...]) + dot_nn(g_up, w_up[...])

                @pl.when(is_mid)
                def _():
                    part[slot, :, pl.ds(0, d_model)] = g_norm

                @pl.when(is_end)
                def _():
                    @pl.when(idx >= 2)
                    def _():
                        part_copy(at(idx - 2), slot + 2).wait_send()

                    p_out[slot + 2] = g_norm.astype(BF16)
                    part_copy(idx, slot + 2).start()

        @pl.when(step < units)
        def _():
            idx = at(step)

            @pl.when(is_end)
            def _():
                c_copy(idx).wait_recv()

            mask_rows = mask[idx]
            g_low = gld_s[...]
            g_a_down[...] += dot_tn(g_low, q_s[...])[:used]
            g_b_up[...] += dot_tn(low_s[idx], gup_s[...])[:used]
            g_b_down[...] += dot_tn(unfold(c_s[idx], mask_rows), g_in[idx])[:used]

        @pl.when(step >= 3)
        def _():
            unit = at(step - 3)

            @pl.when(is_end)
            def _():
                l_copy(unit).wait_recv()

            _, normed = normed_of(h_in[unit].astype(F32))
            g_a_up[...] += dot_tn(unfold(l_s[unit], mask[unit]), normed)[:used]

        return carry

    lax.fori_loop(0, units + 3, bwd_iter, 0)
    g_b_up[...] = LORA_SCALE * g_b_up[...]
    g_b_down[...] = LORA_SCALE * g_b_down[...]

    @pl.when(is_mid & is_last)
    def _():
        loss_copy_same().start()

    @pl.when(jnp.logical_not(is_mid & is_last))
    def _():
        loss_copy(0).wait_recv()
        loss_out[...] = loss_in[...]

    @pl.when(is_mid & (stage > 0))
    def _():
        loss_copy(0).start()
        loss_copy(1).start()

    @pl.when(is_mid & is_last)
    def _():
        loss_copy_same().wait_send()

    @pl.when(is_mid & (stage > 0))
    def _():
        loss_copy(0).wait_send()
        loss_copy(1).wait_send()

    for unit in (units - 2, units - 1):
        slot = jnp.int32(unit % 2)

        @pl.when(is_end)
        def _():
            part_copy(unit, slot).wait_send()
            part_low_copy(unit, slot).wait_send()
            part_low_copy(unit, slot + 2).wait_send()

            @pl.when(stage > 0)
            def _():
                part_copy(unit, slot + 2).wait_send()

        @pl.when(is_mid)
        def _():
            sum_copy(unit, slot).wait_send()
            sum_low_copy(unit, slot).wait_send()
            sum_low_copy(unit, slot + 2).wait_send()

            @pl.when(stage < last)
            def _():
                hidden_copy(unit, slot, 0).wait_send()
                hidden_copy(unit, slot, 1).wait_send()

            @pl.when(stage > 0)
            def _():
                sum_copy(unit, slot + 2).wait_send()
                grad_copy(unit, slot + 2, 0).wait_send()
                grad_copy(unit, slot + 2, 1).wait_send()

    @pl.when(is_mid)
    def _():
        def drain(idx, carry):
            c_copy(idx).wait_send()
            l_copy(idx).wait_send()

            @pl.when(is_last)
            def _():
                top_copy(idx).wait_send()

            return carry

        lax.fori_loop(0, units, drain, 0)


def sweep(units, stages, weights, rows, mask, weight, collective_id):
    width, d_model = weights[0].shape
    used = weights[4].shape[0]
    msg = d_model + FOLD
    vmem = pl.BlockSpec(memory_space=pltpu.VMEM)
    out_shape = (
        jax.ShapeDtypeStruct((8, LANES), F32),
        jax.ShapeDtypeStruct((used, d_model), F32),
        jax.ShapeDtypeStruct((used, width), F32),
        jax.ShapeDtypeStruct((used, width), F32),
        jax.ShapeDtypeStruct((used, d_model), F32),
    )
    dma = pltpu.SemaphoreType.DMA
    return pl.pallas_call(
        functools.partial(sweep_kernel, units, stages),
        out_shape=out_shape,
        in_specs=[vmem] * 4 + [pl.BlockSpec(memory_space=pltpu.HBM)] * 5 + [vmem] * 2,
        out_specs=(vmem,) * 5,
        scratch_shapes=[
            pltpu.VMEM((units, UNIT, d_model), BF16),
            pltpu.VMEM((units, UNIT, d_model), BF16),
            pltpu.VMEM((units, UNIT, width), F32),
            pltpu.VMEM((units, UNIT, width), F32),
            pltpu.VMEM((units, UNIT, LANES), BF16),
            pltpu.VMEM((units, UNIT, FOLD), BF16),
            pltpu.VMEM((units, UNIT, FOLD), BF16),
            pltpu.VMEM((units, UNIT, d_model), BF16),
            pltpu.VMEM((units, UNIT, FOLD), BF16),
            pltpu.VMEM((2 * units, UNIT, d_model), BF16),
            pltpu.VMEM((2 * units, UNIT, FOLD), BF16),
            pltpu.VMEM((2, UNIT, msg), F32),
            pltpu.VMEM((4, UNIT, d_model), BF16),
            pltpu.VMEM((4, UNIT, FOLD), BF16),
            pltpu.VMEM((4, UNIT, d_model), BF16),
            pltpu.VMEM((4, UNIT, FOLD), BF16),
            pltpu.VMEM((4, UNIT, d_model), BF16),
            pltpu.VMEM((UNIT, width), BF16),
            pltpu.VMEM((UNIT, width), BF16),
            pltpu.VMEM((UNIT, LANES), BF16),
            pltpu.VMEM((8, LANES), F32),
            pltpu.VMEM((LANES, d_model), BF16),
            pltpu.VMEM((LANES, width), BF16),
            pltpu.VMEM((LANES, width), BF16),
            pltpu.VMEM((LANES, d_model), BF16),
            dma,
            dma((4,)),
            dma((units,)),
            dma((units,)),
            dma((2 * units,)),
            dma((2 * units,)),
            dma((units,)),
            dma((units,)),
            dma((units,)),
            dma((units,)),
            dma,
            dma((4,)),
            dma((4,)),
            dma((4,)),
            dma((4,)),
            dma((4, 2)),
            dma((units,)),
            dma((units,)),
            dma((units,)),
            dma((3,)),
        ],
        compiler_params=pltpu.CompilerParams(collective_id=collective_id, has_side_effects=True,
                                             vmem_limit_bytes=66_000_000),
    )(*weights, rows, mask, weight)


def solution(mesh):
    num_stages = mesh.shape["pp"]

    def stage_body(w_gate, w_up, w_down, norm_gain, a_up, b_up, a_down, b_down, inputs, targets, lengths):
        stage_idx = lax.axis_index("pp")
        num_jobs, num_micro, row_count, seq_len, d_model = inputs.shape
        rank = a_up.shape[-1]
        job_rows = num_micro * row_count
        num_rows = num_jobs * job_rows
        num_tokens = num_rows * seq_len
        width = w_gate.shape[-1]
        used = num_jobs * rank

        order = np.arange(num_rows).reshape(lengths.shape)
        row_lens = jnp.sum(jnp.where(np.arange(num_rows)[:, None, None, None] == order[None], lengths[None], 0), axis=(1, 2, 3))
        row_ends = jnp.cumsum(row_lens)
        row_starts = row_ends - row_lens
        job_norms = jnp.sum(lengths, axis=(1, 2)).astype(F32) * d_model
        row_jobs = jnp.arange(num_rows) // job_rows
        row_shift = jnp.arange(num_rows) * seq_len - row_starts
        row_weight = jnp.repeat(1.0 / job_norms, job_rows)

        a_up_all = jnp.swapaxes(a_up[0], 1, 2).reshape(used, d_model)
        b_up_all = b_up[0].reshape(used, width)
        a_down_all = jnp.swapaxes(a_down[0], 1, 2).reshape(used, width)
        b_down_all = b_down[0].reshape(used, d_model)
        gain = jnp.broadcast_to(norm_gain.astype(F32), (UNIT, d_model))
        weights = (jnp.swapaxes(w_gate[0], 0, 1), jnp.swapaxes(w_up[0], 0, 1), w_down[0], gain, a_up_all, b_up_all, a_down_all, b_down_all)
        rows_all = jnp.where(stage_idx == num_stages - 1, targets, inputs).reshape(num_tokens, d_model)

        def run(plan):
            def one_pass(units, first):
                slots = first + jnp.arange(units * UNIT)
                in_row = (slots[:, None] >= row_starts[None, :]) & (slots[:, None] < row_ends[None, :])
                valid = slots < row_ends[-1]
                source = slots + jnp.sum(jnp.where(in_row, row_shift[None, :], 0), axis=1)
                job = jnp.sum(jnp.where(in_row, row_jobs[None, :], 0), axis=1)
                weight = jnp.sum(jnp.where(in_row, row_weight[None, :], 0.0), axis=1)
                pick = ((source[:, None] == jnp.arange(num_tokens)[None, :]) & valid[:, None]).astype(BF16)
                rows = jnp.dot(pick, rows_all, preferred_element_type=F32).astype(BF16)
                mask = ((jnp.arange(LANES)[None, :] // rank == job[:, None]) & valid[:, None]).astype(BF16)
                return sweep(units, num_stages, weights,
                             rows.reshape(units, UNIT, d_model), mask.reshape(units, UNIT, LANES),
                             jnp.broadcast_to(weight[:, None], (units * UNIT, FOLD)).reshape(units, UNIT, FOLD), 0)

            if len(plan) == 1:
                return tuple(one_pass(plan[0], 0))
            zeros = tuple(jnp.zeros(shape, F32) for shape in ((8, LANES), (used, d_model), (used, width), (used, width), (used, d_model)))
            return lax.fori_loop(0, len(plan), lambda turn, outs: tuple(
                old + add for old, add in zip(outs, one_pass(plan[0], turn * plan[0] * UNIT))), zeros)

        caps = [sum(plan) * UNIT for plan in PLANS]
        choice = sum((row_ends[-1] > cap).astype(jnp.int32) for cap in caps[:-1])
        loss, g_a_up, g_b_up, g_a_down, g_b_down = lax.switch(choice, [functools.partial(run, plan) for plan in PLANS])
        losses = 0.5 * loss[0, :used:rank]
        g_a_up = jnp.swapaxes(g_a_up.reshape(1, num_jobs, rank, d_model), 2, 3)
        g_b_up = g_b_up.reshape(1, num_jobs, rank, width)
        g_a_down = jnp.swapaxes(g_a_down.reshape(1, num_jobs, rank, width), 2, 3)
        g_b_down = g_b_down.reshape(1, num_jobs, rank, d_model)
        return losses, g_a_up, g_b_up, g_a_down, g_b_down

    weight_specs = (P("pp", None, "tp"), P("pp", None, "tp"), P("pp", "tp", None), P("pp", None))
    adapter_specs = (P("pp", "rep", None, None), P("pp", "rep", None, "tp"), P("pp", "rep", "tp", None), P("pp", "rep", None, None))
    data_specs = (P("rep"), P("rep"), P("rep"))
    return jax.shard_map(stage_body, mesh=mesh, in_specs=weight_specs + adapter_specs + data_specs,
                         out_specs=(P("rep"),) + adapter_specs, check_vma=False)
```

```python
import functools

import jax
import jax.numpy as jnp
import numpy as np
from jax import lax
from jax.experimental import pallas as pl
from jax.experimental.pallas import tpu as pltpu
from jax.sharding import PartitionSpec as P

LORA_SCALE = 2.0
NORM_EPS = 1e-5
UNIT = 128
LANES = 256
FOLD = 128
PLANS = ((10,), (12,), (9, 9))
MESH_ID = pl.DeviceIdType.MESH
F32 = jnp.float32
BF16 = jnp.bfloat16


def dot_nn(lhs, rhs):
    return lax.dot_general(lhs, rhs, (((1,), (0,)), ((), ())), preferred_element_type=F32)


def dot_nt(lhs, rhs):
    return lax.dot_general(lhs, rhs, (((1,), (1,)), ((), ())), preferred_element_type=F32)


def dot_tn(lhs, rhs):
    return lax.dot_general(lhs, rhs, (((0,), (0,)), ((), ())), preferred_element_type=F32)


def fold(wide):
    return wide[:, :FOLD] + wide[:, FOLD:]


def unfold(folded, mask):
    return jnp.concatenate([folded, folded], axis=1) * mask


def sweep_kernel(units, stages,
                 w_gate, w_up, w_down, gain, a_up_hbm, b_up_hbm, a_down_hbm, b_down_hbm, rows_hbm, mask, weight,
                 loss_out, g_a_up, g_b_up, g_a_down, g_b_down,
                 h_in, g_in, gate_s, up_s, low_s, c_s, l_s, p_in, pl_in, s_in, sl_in, part, p_out, pl_out, s_out, sl_out, h_out, q_s, gup_s, ggate_s, gld_s, loss_in,
                 a_up, b_up, a_down, b_down, load_sem, adapter_sem, p_sem, pl_sem, s_sem, sl_sem, h_sem, g_sem, c_sem, l_sem, loss_sem,
                 p_send, pl_send, s_send, sl_send, h_send, c_send, l_send, g_send, loss_send):
    d_model = h_in.shape[2]
    used = g_a_up.shape[0]
    tp_idx = lax.axis_index("tp")
    stage = lax.axis_index("pp")
    last = stages - 1
    is_mid = lax.div(tp_idx + 1, 2) == 1
    is_end = lax.div(tp_idx + 1, 2) != 1
    mid_idx = 1 + lax.div(tp_idx, 2)
    end_idx = 3 * lax.div(tp_idx, 2)
    later = lax.rem(stage + 1, stages)
    earlier = lax.rem(stage + stages - 1, stages)
    cross_idx = 3 - tp_idx
    is_first = stage == 0
    is_last = stage == last

    def remote(src, dst, send, recv, tp_to, pp_to):
        return pltpu.make_async_remote_copy(src_ref=src, dst_ref=dst, send_sem=send, recv_sem=recv,
                                            device_id={"tp": tp_to, "pp": pp_to}, device_id_type=MESH_ID)

    load_inputs = pltpu.make_async_copy(rows_hbm, h_in, load_sem)
    load_targets = pltpu.make_async_copy(rows_hbm, g_in, load_sem)

    @pl.when(is_first)
    def _():
        load_inputs.start()

    @pl.when(is_last & is_mid)
    def _():
        load_targets.start()

    adapters = [(a_up_hbm, a_up), (b_up_hbm, b_up), (a_down_hbm, a_down), (b_down_hbm, b_down)]
    adapter_loads = [pltpu.make_async_copy(src, dst.at[pl.ds(0, used)], adapter_sem.at[which])
                     for which, (src, dst) in enumerate(adapters)]
    for load in adapter_loads:
        load.start()
    for _, dst in adapters:
        dst[pl.ds(used, LANES - used), :] = jnp.zeros((LANES - used, dst.shape[1]), BF16)

    barrier = pltpu.get_barrier_semaphore()

    def greet(tp_to, pp_to):
        pl.semaphore_signal(barrier, inc=1, device_id={"tp": tp_to, "pp": pp_to}, device_id_type=MESH_ID)

    @pl.when(is_mid)
    def _():
        greet(end_idx, stage)
        greet(cross_idx, stage)

        @pl.when(stage < last)
        def _():
            greet(mid_idx, later)
            greet(end_idx, later)

        @pl.when(stage > 0)
        def _():
            greet(mid_idx, earlier)
            greet(end_idx, earlier)

        pl.semaphore_wait(barrier, 2 + 2 * (stage < last).astype(jnp.int32) + 2 * (stage > 0).astype(jnp.int32))

    @pl.when(is_end)
    def _():
        greet(mid_idx, stage)

        @pl.when(stage < last)
        def _():
            greet(mid_idx, later)

        @pl.when(stage > 0)
        def _():
            greet(mid_idx, earlier)

        pl.semaphore_wait(barrier, 1 + (stage < last).astype(jnp.int32) + (stage > 0).astype(jnp.int32))

    loss_out[...] = jnp.zeros_like(loss_out)
    g_a_up[...] = jnp.zeros_like(g_a_up)
    g_b_up[...] = jnp.zeros_like(g_b_up)
    g_a_down[...] = jnp.zeros_like(g_a_down)
    g_b_down[...] = jnp.zeros_like(g_b_down)

    for load in adapter_loads:
        load.wait()

    @pl.when(is_first)
    def _():
        load_inputs.wait()

    @pl.when(is_last & is_mid)
    def _():
        load_targets.wait()

    def part_copy(idx, slot):
        return remote(p_out.at[slot], p_in.at[idx], p_send.at[slot], p_sem.at[idx], mid_idx, stage)

    def part_low_copy(idx, slot):
        return remote(pl_out.at[slot], pl_in.at[idx], pl_send.at[slot], pl_sem.at[idx], mid_idx, stage)

    def sum_copy(idx, slot):
        land = 2 * idx + lax.div(slot, 2)
        return remote(s_out.at[slot], s_in.at[land], s_send.at[slot], s_sem.at[land], cross_idx, stage)

    def sum_low_copy(idx, slot):
        land = 2 * idx + lax.div(slot, 2)
        return remote(sl_out.at[slot], sl_in.at[land], sl_send.at[slot], sl_sem.at[land], cross_idx, stage)

    def hidden_copy(idx, slot, which):
        return remote(h_out.at[slot], h_in.at[idx], h_send.at[slot, which], h_sem.at[idx],
                      (mid_idx, end_idx)[which], later)

    def grad_copy(idx, slot, which):
        return remote(h_out.at[slot], g_in.at[idx], h_send.at[slot, which], g_sem.at[idx],
                      (mid_idx, end_idx)[which], earlier)

    def top_copy(idx):
        return remote(g_in.at[idx], g_in.at[idx], g_send.at[idx], g_sem.at[idx], end_idx, stage)

    def c_copy(idx):
        return remote(c_s.at[idx], c_s.at[idx], c_send.at[idx], c_sem.at[idx], end_idx, stage)

    def l_copy(idx):
        return remote(l_s.at[idx], l_s.at[idx], l_send.at[idx], l_sem.at[idx], end_idx, stage)

    def loss_copy(which):
        return remote(loss_out, loss_in, loss_send.at[which], loss_sem,
                      (mid_idx, end_idx)[which], earlier)

    def loss_copy_same():
        return remote(loss_out, loss_in, loss_send.at[2], loss_sem, end_idx, stage)

    def normed_of(hidden_f32):
        inv_rms = lax.rsqrt(jnp.mean(hidden_f32 * hidden_f32, axis=-1, keepdims=True) + NORM_EPS)
        return inv_rms, (hidden_f32 * inv_rms * gain[...]).astype(BF16)

    def at(unit):
        return jnp.clip(unit, 0, units - 1)

    def fwd_iter(step, carry):
        @pl.when(step < units)
        def _():
            idx = at(step)
            slot = lax.rem(idx, 2)

            @pl.when(stage > 0)
            def _():
                hidden_copy(idx, slot, 0).wait_recv()

            _, normed = normed_of(h_in[idx].astype(F32))
            mask_rows = mask[idx]
            low = dot_nt(normed, a_up[...]).astype(BF16) * mask_rows
            low_s[idx] = low
            gate_pre = dot_nt(normed, w_gate[...])
            gate_s[idx] = gate_pre
            up_val = dot_nt(normed, w_up[...]) + LORA_SCALE * dot_nn(low, b_up[...])
            up_s[idx] = up_val
            q_s[...] = (gate_pre * jax.nn.sigmoid(gate_pre) * up_val).astype(BF16)

        @pl.when(is_mid & (step >= 2))
        def _():
            unit = at(step - 2)
            slot = lax.rem(unit, 2)
            sum_copy(unit, slot).wait_recv()
            sum_low_copy(unit, slot).wait_recv()
            total = s_out[slot].astype(F32) + s_in[2 * unit].astype(F32)
            c_fold = (sl_out[slot].astype(F32) + sl_in[2 * unit].astype(F32)).astype(BF16)
            c_s[unit] = c_fold
            c_copy(unit).start()
            mask_rows = mask[unit]
            delta = total + LORA_SCALE * dot_nn(unfold(c_fold, mask_rows), b_down[...])
            hidden = (h_in[unit].astype(F32) + delta).astype(BF16)

            @pl.when(stage < last)
            def _():
                @pl.when(unit >= 2)
                def _():
                    hidden_copy(at(unit - 2), slot, 0).wait_send()
                    hidden_copy(at(unit - 2), slot, 1).wait_send()

                h_out[slot] = hidden
                hidden_copy(unit, slot, 0).start()
                hidden_copy(unit, slot, 1).start()

            @pl.when(is_last)
            def _():
                residual = hidden.astype(F32) - g_in[unit].astype(F32)
                weighted = weight[unit][:, :1] * residual
                g_in[unit] = weighted.astype(BF16)
                top_copy(unit).start()
                row_sum = jnp.sum(weighted * residual, axis=-1, keepdims=True)
                loss_out[...] += jnp.broadcast_to(
                    jnp.sum(row_sum * mask_rows.astype(F32), axis=0, keepdims=True), loss_out.shape)

        @pl.when(is_mid & (step >= 1) & (step <= units))
        def _():
            unit = at(step - 1)
            slot = lax.rem(unit, 2)
            part_copy(unit, slot).wait_recv()
            part_low_copy(unit, slot).wait_recv()

            @pl.when(unit >= 2)
            def _():
                sum_copy(at(unit - 2), slot).wait_send()
                sum_low_copy(at(unit - 2), slot).wait_send()

            s_out[slot] = (part[slot, :, pl.ds(0, d_model)] + p_in[unit].astype(F32)).astype(BF16)
            sum_copy(unit, slot).start()
            sl_out[slot] = (part[slot, :, pl.ds(d_model, FOLD)] + pl_in[unit].astype(F32)).astype(BF16)
            sum_low_copy(unit, slot).start()

        @pl.when(step < units)
        def _():
            idx = at(step)
            slot = lax.rem(idx, 2)
            prod = q_s[...]
            down = dot_nn(prod, w_down[...])
            low_down = fold(dot_nt(prod, a_down[...]) * mask[idx].astype(F32))

            @pl.when(is_mid)
            def _():
                part[slot, :, pl.ds(0, d_model)] = down
                part[slot, :, pl.ds(d_model, FOLD)] = low_down

            @pl.when(is_end)
            def _():
                @pl.when(idx >= 2)
                def _():
                    part_copy(at(idx - 2), slot).wait_send()
                    part_low_copy(at(idx - 2), slot).wait_send()

                p_out[slot] = down.astype(BF16)
                part_copy(idx, slot).start()
                pl_out[slot] = low_down.astype(BF16)
                part_low_copy(idx, slot).start()

        return carry

    lax.fori_loop(0, units + 2, fwd_iter, 0)

    def bwd_iter(step, carry):
        @pl.when(step < units)
        def _():
            idx = at(step)
            slot = lax.rem(idx, 2)

            @pl.when(jnp.logical_not(is_last & is_mid))
            def _():
                grad_copy(idx, slot + 2, 0).wait_recv()

            grad = g_in[idx]
            mask_rows = mask[idx]
            g_low = (LORA_SCALE * dot_nt(grad, b_down[...])).astype(BF16) * mask_rows
            gld_s[...] = g_low
            g_prod = dot_nt(grad, w_down[...]) + dot_nn(g_low, a_down[...])
            gate_pre = gate_s[idx]
            up_val = up_s[idx]
            sig = jax.nn.sigmoid(gate_pre)
            act = gate_pre * sig
            q_s[...] = (act * up_val).astype(BF16)
            g_up = (g_prod * act).astype(BF16)
            gup_s[...] = g_up
            ggate_s[...] = (g_prod * up_val * (sig * (1.0 + gate_pre * (1.0 - sig)))).astype(BF16)
            g_low_up = fold(dot_nt(g_up, b_up[...]) * mask_rows.astype(F32))

            @pl.when(is_mid)
            def _():
                part[slot, :, pl.ds(d_model, FOLD)] = g_low_up

            @pl.when(is_end)
            def _():
                @pl.when(idx >= 2)
                def _():
                    part_low_copy(at(idx - 2), slot + 2).wait_send()

                pl_out[slot + 2] = g_low_up.astype(BF16)
                part_low_copy(idx, slot + 2).start()

        @pl.when(is_mid & (step >= 2) & (step <= units + 1))
        def _():
            unit = at(step - 2)
            slot = lax.rem(unit, 2)
            sum_low_copy(unit, slot + 2).wait_recv()
            low_total = sl_out[slot + 2].astype(F32) + sl_in[2 * unit + 1].astype(F32)
            l_fold = (LORA_SCALE * low_total).astype(BF16)
            l_s[unit] = l_fold
            l_copy(unit).start()

            @pl.when(stage > 0)
            def _():
                sum_copy(unit, slot + 2).wait_recv()
                total = s_out[slot + 2].astype(F32) + s_in[2 * unit + 1].astype(F32)
                g_normed = total + dot_nn(unfold(l_fold, mask[unit]), a_up[...])
                hidden_f32 = h_in[unit].astype(F32)
                inv_rms = lax.rsqrt(jnp.mean(hidden_f32 * hidden_f32, axis=-1, keepdims=True) + NORM_EPS)
                g_scaled = g_normed * gain[...]
                unit_rows = hidden_f32 * inv_rms
                g_hidden = inv_rms * (g_scaled - unit_rows * jnp.mean(g_scaled * unit_rows, axis=-1, keepdims=True))

                @pl.when(unit >= 2)
                def _():
                    grad_copy(at(unit - 2), slot + 2, 0).wait_send()
                    grad_copy(at(unit - 2), slot + 2, 1).wait_send()

                h_out[slot + 2] = (g_in[unit].astype(F32) + g_hidden).astype(BF16)
                grad_copy(unit, slot + 2, 0).start()
                grad_copy(unit, slot + 2, 1).start()

        @pl.when(is_mid & (step >= 1) & (step <= units))
        def _():
            unit = at(step - 1)
            slot = lax.rem(unit, 2)
            part_low_copy(unit, slot + 2).wait_recv()

            @pl.when(unit >= 2)
            def _():
                sum_low_copy(at(unit - 2), slot + 2).wait_send()

            sl_out[slot + 2] = (part[slot, :, pl.ds(d_model, FOLD)] + pl_in[unit].astype(F32)).astype(BF16)
            sum_low_copy(unit, slot + 2).start()

            @pl.when(stage > 0)
            def _():
                part_copy(unit, slot + 2).wait_recv()

                @pl.when(unit >= 2)
                def _():
                    sum_copy(at(unit - 2), slot + 2).wait_send()

                s_out[slot + 2] = (part[slot, :, pl.ds(0, d_model)] + p_in[unit].astype(F32)).astype(BF16)
                sum_copy(unit, slot + 2).start()

        @pl.when(step < units)
        def _():
            idx = at(step)
            slot = lax.rem(idx, 2)

            @pl.when(stage > 0)
            def _():
                g_gate = ggate_s[...]
                g_up = gup_s[...]
                g_norm = dot_nn(g_gate, w_gate[...]) + dot_nn(g_up, w_up[...])

                @pl.when(is_mid)
                def _():
                    part[slot, :, pl.ds(0, d_model)] = g_norm

                @pl.when(is_end)
                def _():
                    @pl.when(idx >= 2)
                    def _():
                        part_copy(at(idx - 2), slot + 2).wait_send()

                    p_out[slot + 2] = g_norm.astype(BF16)
                    part_copy(idx, slot + 2).start()

        @pl.when(step < units)
        def _():
            idx = at(step)

            @pl.when(is_end)
            def _():
                c_copy(idx).wait_recv()

            mask_rows = mask[idx]
            g_low = gld_s[...]
            g_a_down[...] += dot_tn(g_low, q_s[...])[:used]
            g_b_up[...] += dot_tn(low_s[idx], gup_s[...])[:used]
            g_b_down[...] += dot_tn(unfold(c_s[idx], mask_rows), g_in[idx])[:used]

        @pl.when(step >= 3)
        def _():
            unit = at(step - 3)

            @pl.when(is_end)
            def _():
                l_copy(unit).wait_recv()

            _, normed = normed_of(h_in[unit].astype(F32))
            g_a_up[...] += dot_tn(unfold(l_s[unit], mask[unit]), normed)[:used]

        return carry

    lax.fori_loop(0, units + 3, bwd_iter, 0)
    g_b_up[...] = LORA_SCALE * g_b_up[...]
    g_b_down[...] = LORA_SCALE * g_b_down[...]

    @pl.when(is_mid & is_last)
    def _():
        loss_copy_same().start()

    @pl.when(jnp.logical_not(is_mid & is_last))
    def _():
        loss_copy(0).wait_recv()
        loss_out[...] = loss_in[...]

    @pl.when(is_mid & (stage > 0))
    def _():
        loss_copy(0).start()
        loss_copy(1).start()

    @pl.when(is_mid & is_last)
    def _():
        loss_copy_same().wait_send()

    @pl.when(is_mid & (stage > 0))
    def _():
        loss_copy(0).wait_send()
        loss_copy(1).wait_send()

    for unit in (units - 2, units - 1):
        slot = jnp.int32(unit % 2)

        @pl.when(is_end)
        def _():
            part_copy(unit, slot).wait_send()
            part_low_copy(unit, slot).wait_send()
            part_low_copy(unit, slot + 2).wait_send()

            @pl.when(stage > 0)
            def _():
                part_copy(unit, slot + 2).wait_send()

        @pl.when(is_mid)
        def _():
            sum_copy(unit, slot).wait_send()
            sum_low_copy(unit, slot).wait_send()
            sum_low_copy(unit, slot + 2).wait_send()

            @pl.when(stage < last)
            def _():
                hidden_copy(unit, slot, 0).wait_send()
                hidden_copy(unit, slot, 1).wait_send()

            @pl.when(stage > 0)
            def _():
                sum_copy(unit, slot + 2).wait_send()
                grad_copy(unit, slot + 2, 0).wait_send()
                grad_copy(unit, slot + 2, 1).wait_send()

    @pl.when(is_mid)
    def _():
        def drain(idx, carry):
            c_copy(idx).wait_send()
            l_copy(idx).wait_send()

            @pl.when(is_last)
            def _():
                top_copy(idx).wait_send()

            return carry

        lax.fori_loop(0, units, drain, 0)


def sweep(units, stages, weights, rows, mask, weight, collective_id):
    width, d_model = weights[0].shape
    used = weights[4].shape[0]
    msg = d_model + FOLD
    vmem = pl.BlockSpec(memory_space=pltpu.VMEM)
    out_shape = (
        jax.ShapeDtypeStruct((8, LANES), F32),
        jax.ShapeDtypeStruct((used, d_model), F32),
        jax.ShapeDtypeStruct((used, width), F32),
        jax.ShapeDtypeStruct((used, width), F32),
        jax.ShapeDtypeStruct((used, d_model), F32),
    )
    dma = pltpu.SemaphoreType.DMA
    return pl.pallas_call(
        functools.partial(sweep_kernel, units, stages),
        out_shape=out_shape,
        in_specs=[vmem] * 4 + [pl.BlockSpec(memory_space=pltpu.HBM)] * 5 + [vmem] * 2,
        out_specs=(vmem,) * 5,
        scratch_shapes=[
            pltpu.VMEM((units, UNIT, d_model), BF16),
            pltpu.VMEM((units, UNIT, d_model), BF16),
            pltpu.VMEM((units, UNIT, width), F32),
            pltpu.VMEM((units, UNIT, width), F32),
            pltpu.VMEM((units, UNIT, LANES), BF16),
            pltpu.VMEM((units, UNIT, FOLD), BF16),
            pltpu.VMEM((units, UNIT, FOLD), BF16),
            pltpu.VMEM((units, UNIT, d_model), BF16),
            pltpu.VMEM((units, UNIT, FOLD), BF16),
            pltpu.VMEM((2 * units, UNIT, d_model), BF16),
            pltpu.VMEM((2 * units, UNIT, FOLD), BF16),
            pltpu.VMEM((2, UNIT, msg), F32),
            pltpu.VMEM((4, UNIT, d_model), BF16),
            pltpu.VMEM((4, UNIT, FOLD), BF16),
            pltpu.VMEM((4, UNIT, d_model), BF16),
            pltpu.VMEM((4, UNIT, FOLD), BF16),
            pltpu.VMEM((4, UNIT, d_model), BF16),
            pltpu.VMEM((UNIT, width), BF16),
            pltpu.VMEM((UNIT, width), BF16),
            pltpu.VMEM((UNIT, width), BF16),
            pltpu.VMEM((UNIT, LANES), BF16),
            pltpu.VMEM((8, LANES), F32),
            pltpu.VMEM((LANES, d_model), BF16),
            pltpu.VMEM((LANES, width), BF16),
            pltpu.VMEM((LANES, width), BF16),
            pltpu.VMEM((LANES, d_model), BF16),
            dma,
            dma((4,)),
            dma((units,)),
            dma((units,)),
            dma((2 * units,)),
            dma((2 * units,)),
            dma((units,)),
            dma((units,)),
            dma((units,)),
            dma((units,)),
            dma,
            dma((4,)),
            dma((4,)),
            dma((4,)),
            dma((4,)),
            dma((4, 2)),
            dma((units,)),
            dma((units,)),
            dma((units,)),
            dma((3,)),
        ],
        compiler_params=pltpu.CompilerParams(collective_id=collective_id, has_side_effects=True,
                                             vmem_limit_bytes=66_000_000),
    )(*weights, rows, mask, weight)


def solution(mesh):
    num_stages = mesh.shape["pp"]

    def stage_body(w_gate, w_up, w_down, norm_gain, a_up, b_up, a_down, b_down, inputs, targets, lengths):
        stage_idx = lax.axis_index("pp")
        num_jobs, num_micro, row_count, seq_len, d_model = inputs.shape
        rank = a_up.shape[-1]
        job_rows = num_micro * row_count
        num_rows = num_jobs * job_rows
        num_tokens = num_rows * seq_len
        width = w_gate.shape[-1]
        used = num_jobs * rank

        order = np.arange(num_rows).reshape(lengths.shape)
        row_lens = jnp.sum(jnp.where(np.arange(num_rows)[:, None, None, None] == order[None], lengths[None], 0), axis=(1, 2, 3))
        row_ends = jnp.cumsum(row_lens)
        row_starts = row_ends - row_lens
        job_norms = jnp.sum(lengths, axis=(1, 2)).astype(F32) * d_model
        row_jobs = jnp.arange(num_rows) // job_rows
        row_shift = jnp.arange(num_rows) * seq_len - row_starts
        row_weight = jnp.repeat(1.0 / job_norms, job_rows)

        a_up_all = jnp.swapaxes(a_up[0], 1, 2).reshape(used, d_model)
        b_up_all = b_up[0].reshape(used, width)
        a_down_all = jnp.swapaxes(a_down[0], 1, 2).reshape(used, width)
        b_down_all = b_down[0].reshape(used, d_model)
        gain = jnp.broadcast_to(norm_gain.astype(F32), (UNIT, d_model))
        weights = (jnp.swapaxes(w_gate[0], 0, 1), jnp.swapaxes(w_up[0], 0, 1), w_down[0], gain, a_up_all, b_up_all, a_down_all, b_down_all)
        rows_all = jnp.where(stage_idx == num_stages - 1, targets, inputs).reshape(num_tokens, d_model)

        def run(plan):
            def one_pass(units, first):
                slots = first + jnp.arange(units * UNIT)
                in_row = (slots[:, None] >= row_starts[None, :]) & (slots[:, None] < row_ends[None, :])
                valid = slots < row_ends[-1]
                source = slots + jnp.sum(jnp.where(in_row, row_shift[None, :], 0), axis=1)
                job = jnp.sum(jnp.where(in_row, row_jobs[None, :], 0), axis=1)
                weight = jnp.sum(jnp.where(in_row, row_weight[None, :], 0.0), axis=1)
                pick = ((source[:, None] == jnp.arange(num_tokens)[None, :]) & valid[:, None]).astype(BF16)
                rows = jnp.dot(pick, rows_all, preferred_element_type=F32).astype(BF16)
                mask = ((jnp.arange(LANES)[None, :] // rank == job[:, None]) & valid[:, None]).astype(BF16)
                return sweep(units, num_stages, weights,
                             rows.reshape(units, UNIT, d_model), mask.reshape(units, UNIT, LANES),
                             jnp.broadcast_to(weight[:, None], (units * UNIT, FOLD)).reshape(units, UNIT, FOLD), 0)

            if len(plan) == 1:
                return tuple(one_pass(plan[0], 0))
            zeros = tuple(jnp.zeros(shape, F32) for shape in ((8, LANES), (used, d_model), (used, width), (used, width), (used, d_model)))
            return lax.fori_loop(0, len(plan), lambda turn, outs: tuple(
                old + add for old, add in zip(outs, one_pass(plan[0], turn * plan[0] * UNIT))), zeros)

        caps = [sum(plan) * UNIT for plan in PLANS]
        choice = sum((row_ends[-1] > cap).astype(jnp.int32) for cap in caps[:-1])
        loss, g_a_up, g_b_up, g_a_down, g_b_down = lax.switch(choice, [functools.partial(run, plan) for plan in PLANS])
        losses = 0.5 * loss[0, :used:rank]
        g_a_up = jnp.swapaxes(g_a_up.reshape(1, num_jobs, rank, d_model), 2, 3)
        g_b_up = g_b_up.reshape(1, num_jobs, rank, width)
        g_a_down = jnp.swapaxes(g_a_down.reshape(1, num_jobs, rank, width), 2, 3)
        g_b_down = g_b_down.reshape(1, num_jobs, rank, d_model)
        return losses, g_a_up, g_b_up, g_a_down, g_b_down

    weight_specs = (P("pp", None, "tp"), P("pp", None, "tp"), P("pp", "tp", None), P("pp", None))
    adapter_specs = (P("pp", "rep", None, None), P("pp", "rep", None, "tp"), P("pp", "rep", "tp", None), P("pp", "rep", None, None))
    data_specs = (P("rep"), P("rep"), P("rep"))
    return jax.shard_map(stage_body, mesh=mesh, in_specs=weight_specs + adapter_specs + data_specs,
                         out_specs=(P("rep"),) + adapter_specs, check_vma=False)
```

```python
import functools

import jax
import jax.numpy as jnp
import numpy as np
from jax import lax
from jax.experimental import pallas as pl
from jax.experimental.pallas import tpu as pltpu
from jax.sharding import PartitionSpec as P

LORA_SCALE = 2.0
NORM_EPS = 1e-5
UNIT = 64
LANES = 256
FOLD = 128
PLANS = ((20,), (24,), (18, 18))
MESH_ID = pl.DeviceIdType.MESH
F32 = jnp.float32
BF16 = jnp.bfloat16


def dot_nn(lhs, rhs):
    return lax.dot_general(lhs, rhs, (((1,), (0,)), ((), ())), preferred_element_type=F32)


def dot_nt(lhs, rhs):
    return lax.dot_general(lhs, rhs, (((1,), (1,)), ((), ())), preferred_element_type=F32)


def dot_tn(lhs, rhs):
    return lax.dot_general(lhs, rhs, (((0,), (0,)), ((), ())), preferred_element_type=F32)


def fold(wide):
    return wide[:, :FOLD] + wide[:, FOLD:]


def unfold(folded, mask):
    return jnp.concatenate([folded, folded], axis=1) * mask


def sweep_kernel(units, stages,
                 w_gate, w_up, w_down, gain, a_up_hbm, b_up_hbm, a_down_hbm, b_down_hbm, rows_hbm, mask, weight,
                 loss_out, g_a_up, g_b_up, g_a_down, g_b_down,
                 h_in, g_in, gate_s, up_s, low_s, c_s, l_s, p_in, pl_in, s_in, sl_in, part, p_out, pl_out, s_out, sl_out, h_out, q_s, gup_s, gld_s, loss_in,
                 a_up, b_up, a_down, b_down, load_sem, adapter_sem, p_sem, pl_sem, s_sem, sl_sem, h_sem, g_sem, c_sem, l_sem, loss_sem,
                 p_send, pl_send, s_send, sl_send, h_send, c_send, l_send, g_send, loss_send):
    d_model = h_in.shape[2]
    used = g_a_up.shape[0]
    tp_idx = lax.axis_index("tp")
    stage = lax.axis_index("pp")
    last = stages - 1
    is_mid = lax.div(tp_idx + 1, 2) == 1
    is_end = lax.div(tp_idx + 1, 2) != 1
    mid_idx = 1 + lax.div(tp_idx, 2)
    end_idx = 3 * lax.div(tp_idx, 2)
    later = lax.rem(stage + 1, stages)
    earlier = lax.rem(stage + stages - 1, stages)
    cross_idx = 3 - tp_idx
    is_first = stage == 0
    is_last = stage == last

    def remote(src, dst, send, recv, tp_to, pp_to):
        return pltpu.make_async_remote_copy(src_ref=src, dst_ref=dst, send_sem=send, recv_sem=recv,
                                            device_id={"tp": tp_to, "pp": pp_to}, device_id_type=MESH_ID)

    load_inputs = pltpu.make_async_copy(rows_hbm, h_in, load_sem)
    load_targets = pltpu.make_async_copy(rows_hbm, g_in, load_sem)

    @pl.when(is_first)
    def _():
        load_inputs.start()

    @pl.when(is_last & is_mid)
    def _():
        load_targets.start()

    adapters = [(a_up_hbm, a_up), (b_up_hbm, b_up), (a_down_hbm, a_down), (b_down_hbm, b_down)]
    adapter_loads = [pltpu.make_async_copy(src, dst.at[pl.ds(0, used)], adapter_sem.at[which])
                     for which, (src, dst) in enumerate(adapters)]
    for load in adapter_loads:
        load.start()
    for _, dst in adapters:
        dst[pl.ds(used, LANES - used), :] = jnp.zeros((LANES - used, dst.shape[1]), BF16)

    barrier = pltpu.get_barrier_semaphore()

    def greet(tp_to, pp_to):
        pl.semaphore_signal(barrier, inc=1, device_id={"tp": tp_to, "pp": pp_to}, device_id_type=MESH_ID)

    @pl.when(is_mid)
    def _():
        greet(end_idx, stage)
        greet(cross_idx, stage)

        @pl.when(stage < last)
        def _():
            greet(mid_idx, later)
            greet(end_idx, later)

        @pl.when(stage > 0)
        def _():
            greet(mid_idx, earlier)
            greet(end_idx, earlier)

        pl.semaphore_wait(barrier, 2 + 2 * (stage < last).astype(jnp.int32) + 2 * (stage > 0).astype(jnp.int32))

    @pl.when(is_end)
    def _():
        greet(mid_idx, stage)

        @pl.when(stage < last)
        def _():
            greet(mid_idx, later)

        @pl.when(stage > 0)
        def _():
            greet(mid_idx, earlier)

        pl.semaphore_wait(barrier, 1 + (stage < last).astype(jnp.int32) + (stage > 0).astype(jnp.int32))

    loss_out[...] = jnp.zeros_like(loss_out)
    g_a_up[...] = jnp.zeros_like(g_a_up)
    g_b_up[...] = jnp.zeros_like(g_b_up)
    g_a_down[...] = jnp.zeros_like(g_a_down)
    g_b_down[...] = jnp.zeros_like(g_b_down)

    for load in adapter_loads:
        load.wait()

    @pl.when(is_first)
    def _():
        load_inputs.wait()

    @pl.when(is_last & is_mid)
    def _():
        load_targets.wait()

    def part_copy(idx, slot):
        return remote(p_out.at[slot], p_in.at[idx], p_send.at[slot], p_sem.at[idx], mid_idx, stage)

    def part_low_copy(idx, slot):
        return remote(pl_out.at[slot], pl_in.at[idx], pl_send.at[slot], pl_sem.at[idx], mid_idx, stage)

    def sum_copy(idx, slot):
        land = 2 * idx + lax.div(slot, 2)
        return remote(s_out.at[slot], s_in.at[land], s_send.at[slot], s_sem.at[land], cross_idx, stage)

    def sum_low_copy(idx, slot):
        land = 2 * idx + lax.div(slot, 2)
        return remote(sl_out.at[slot], sl_in.at[land], sl_send.at[slot], sl_sem.at[land], cross_idx, stage)

    def hidden_copy(idx, slot, which):
        return remote(h_out.at[slot], h_in.at[idx], h_send.at[slot, which], h_sem.at[idx],
                      (mid_idx, end_idx)[which], later)

    def grad_copy(idx, slot, which):
        return remote(h_out.at[slot], g_in.at[idx], h_send.at[slot, which], g_sem.at[idx],
                      (mid_idx, end_idx)[which], earlier)

    def top_copy(idx):
        return remote(g_in.at[idx], g_in.at[idx], g_send.at[idx], g_sem.at[idx], end_idx, stage)

    def c_copy(idx):
        return remote(c_s.at[idx], c_s.at[idx], c_send.at[idx], c_sem.at[idx], end_idx, stage)

    def l_copy(idx):
        return remote(l_s.at[idx], l_s.at[idx], l_send.at[idx], l_sem.at[idx], end_idx, stage)

    def loss_copy(which):
        return remote(loss_out, loss_in, loss_send.at[which], loss_sem,
                      (mid_idx, end_idx)[which], earlier)

    def loss_copy_same():
        return remote(loss_out, loss_in, loss_send.at[2], loss_sem, end_idx, stage)

    def normed_of(hidden_f32):
        inv_rms = lax.rsqrt(jnp.mean(hidden_f32 * hidden_f32, axis=-1, keepdims=True) + NORM_EPS)
        return inv_rms, (hidden_f32 * inv_rms * gain[...]).astype(BF16)

    def at(unit):
        return jnp.clip(unit, 0, units - 1)

    def fwd_iter(step, carry):
        @pl.when(step < units)
        def _():
            idx = at(step)
            slot = lax.rem(idx, 2)

            @pl.when(stage > 0)
            def _():
                hidden_copy(idx, slot, 0).wait_recv()

            _, normed = normed_of(h_in[idx].astype(F32))
            mask_rows = mask[idx]
            low = dot_nt(normed, a_up[...]).astype(BF16) * mask_rows
            low_s[idx] = low
            gate_pre = dot_nt(normed, w_gate[...])
            gate_s[idx] = gate_pre
            up_val = dot_nt(normed, w_up[...]) + LORA_SCALE * dot_nn(low, b_up[...])
            up_s[idx] = up_val
            prod = (gate_pre * jax.nn.sigmoid(gate_pre) * up_val).astype(BF16)
            down = dot_nn(prod, w_down[...])
            low_down = fold(dot_nt(prod, a_down[...]) * mask_rows.astype(F32))

            @pl.when(is_mid)
            def _():
                part[slot, :, pl.ds(0, d_model)] = down
                part[slot, :, pl.ds(d_model, FOLD)] = low_down

            @pl.when(is_end)
            def _():
                @pl.when(idx >= 2)
                def _():
                    part_copy(at(idx - 2), slot).wait_send()
                    part_low_copy(at(idx - 2), slot).wait_send()

                p_out[slot] = down.astype(BF16)
                part_copy(idx, slot).start()
                pl_out[slot] = low_down.astype(BF16)
                part_low_copy(idx, slot).start()

        @pl.when(is_mid & (step >= 1) & (step <= units))
        def _():
            unit = at(step - 1)
            slot = lax.rem(unit, 2)
            part_copy(unit, slot).wait_recv()
            part_low_copy(unit, slot).wait_recv()

            @pl.when(unit >= 2)
            def _():
                sum_copy(at(unit - 2), slot).wait_send()
                sum_low_copy(at(unit - 2), slot).wait_send()

            s_out[slot] = (part[slot, :, pl.ds(0, d_model)] + p_in[unit].astype(F32)).astype(BF16)
            sum_copy(unit, slot).start()
            sl_out[slot] = (part[slot, :, pl.ds(d_model, FOLD)] + pl_in[unit].astype(F32)).astype(BF16)
            sum_low_copy(unit, slot).start()

        @pl.when(is_mid & (step >= 2))
        def _():
            unit = at(step - 2)
            slot = lax.rem(unit, 2)
            sum_copy(unit, slot).wait_recv()
            sum_low_copy(unit, slot).wait_recv()
            total = s_out[slot].astype(F32) + s_in[2 * unit].astype(F32)
            c_fold = (sl_out[slot].astype(F32) + sl_in[2 * unit].astype(F32)).astype(BF16)
            c_s[unit] = c_fold
            c_copy(unit).start()
            mask_rows = mask[unit]
            delta = total + LORA_SCALE * dot_nn(unfold(c_fold, mask_rows), b_down[...])
            hidden = (h_in[unit].astype(F32) + delta).astype(BF16)

            @pl.when(stage < last)
            def _():
                @pl.when(unit >= 2)
                def _():
                    hidden_copy(at(unit - 2), slot, 0).wait_send()
                    hidden_copy(at(unit - 2), slot, 1).wait_send()

                h_out[slot] = hidden
                hidden_copy(unit, slot, 0).start()
                hidden_copy(unit, slot, 1).start()

            @pl.when(is_last)
            def _():
                residual = hidden.astype(F32) - g_in[unit].astype(F32)
                weighted = weight[unit][:, :1] * residual
                g_in[unit] = weighted.astype(BF16)
                top_copy(unit).start()
                row_sum = jnp.sum(weighted * residual, axis=-1, keepdims=True)
                loss_out[...] += jnp.broadcast_to(
                    jnp.sum(row_sum * mask_rows.astype(F32), axis=0, keepdims=True), loss_out.shape)

        return carry

    lax.fori_loop(0, units + 2, fwd_iter, 0)

    def bwd_iter(step, carry):
        @pl.when(step < units)
        def _():
            idx = at(step)
            slot = lax.rem(idx, 2)

            @pl.when(jnp.logical_not(is_last & is_mid))
            def _():
                grad_copy(idx, slot + 2, 0).wait_recv()

            grad = g_in[idx]
            mask_rows = mask[idx]
            g_low = (LORA_SCALE * dot_nt(grad, b_down[...])).astype(BF16) * mask_rows
            gld_s[...] = g_low
            g_prod = dot_nt(grad, w_down[...]) + dot_nn(g_low, a_down[...])
            gate_pre = gate_s[idx]
            up_val = up_s[idx]
            sig = jax.nn.sigmoid(gate_pre)
            act = gate_pre * sig
            q_s[...] = (act * up_val).astype(BF16)
            g_up = (g_prod * act).astype(BF16)
            gup_s[...] = g_up
            g_gate = (g_prod * up_val * (sig * (1.0 + gate_pre * (1.0 - sig)))).astype(BF16)
            g_low_up = fold(dot_nt(g_up, b_up[...]) * mask_rows.astype(F32))

            @pl.when(is_mid)
            def _():
                part[slot, :, pl.ds(d_model, FOLD)] = g_low_up

            @pl.when(is_end)
            def _():
                @pl.when(idx >= 2)
                def _():
                    part_low_copy(at(idx - 2), slot + 2).wait_send()

                pl_out[slot + 2] = g_low_up.astype(BF16)
                part_low_copy(idx, slot + 2).start()

            @pl.when(stage > 0)
            def _():
                g_norm = dot_nn(g_gate, w_gate[...]) + dot_nn(g_up, w_up[...])

                @pl.when(is_mid)
                def _():
                    part[slot, :, pl.ds(0, d_model)] = g_norm

                @pl.when(is_end)
                def _():
                    @pl.when(idx >= 2)
                    def _():
                        part_copy(at(idx - 2), slot + 2).wait_send()

                    p_out[slot + 2] = g_norm.astype(BF16)
                    part_copy(idx, slot + 2).start()

        @pl.when(is_mid & (step >= 1) & (step <= units))
        def _():
            unit = at(step - 1)
            slot = lax.rem(unit, 2)
            part_low_copy(unit, slot + 2).wait_recv()

            @pl.when(unit >= 2)
            def _():
                sum_low_copy(at(unit - 2), slot + 2).wait_send()

            sl_out[slot + 2] = (part[slot, :, pl.ds(d_model, FOLD)] + pl_in[unit].astype(F32)).astype(BF16)
            sum_low_copy(unit, slot + 2).start()

            @pl.when(stage > 0)
            def _():
                part_copy(unit, slot + 2).wait_recv()

                @pl.when(unit >= 2)
                def _():
                    sum_copy(at(unit - 2), slot + 2).wait_send()

                s_out[slot + 2] = (part[slot, :, pl.ds(0, d_model)] + p_in[unit].astype(F32)).astype(BF16)
                sum_copy(unit, slot + 2).start()

        @pl.when(is_mid & (step >= 2) & (step <= units + 1))
        def _():
            unit = at(step - 2)
            slot = lax.rem(unit, 2)
            sum_low_copy(unit, slot + 2).wait_recv()
            low_total = sl_out[slot + 2].astype(F32) + sl_in[2 * unit + 1].astype(F32)
            l_fold = (LORA_SCALE * low_total).astype(BF16)
            l_s[unit] = l_fold
            l_copy(unit).start()

            @pl.when(stage > 0)
            def _():
                sum_copy(unit, slot + 2).wait_recv()
                total = s_out[slot + 2].astype(F32) + s_in[2 * unit + 1].astype(F32)
                g_normed = total + dot_nn(unfold(l_fold, mask[unit]), a_up[...])
                hidden_f32 = h_in[unit].astype(F32)
                inv_rms = lax.rsqrt(jnp.mean(hidden_f32 * hidden_f32, axis=-1, keepdims=True) + NORM_EPS)
                g_scaled = g_normed * gain[...]
                unit_rows = hidden_f32 * inv_rms
                g_hidden = inv_rms * (g_scaled - unit_rows * jnp.mean(g_scaled * unit_rows, axis=-1, keepdims=True))

                @pl.when(unit >= 2)
                def _():
                    grad_copy(at(unit - 2), slot + 2, 0).wait_send()
                    grad_copy(at(unit - 2), slot + 2, 1).wait_send()

                h_out[slot + 2] = (g_in[unit].astype(F32) + g_hidden).astype(BF16)
                grad_copy(unit, slot + 2, 0).start()
                grad_copy(unit, slot + 2, 1).start()

        @pl.when(step < units)
        def _():
            idx = at(step)

            @pl.when(is_end)
            def _():
                c_copy(idx).wait_recv()

            mask_rows = mask[idx]
            g_low = gld_s[...]
            g_a_down[...] += dot_tn(g_low, q_s[...])[:used]
            g_b_up[...] += dot_tn(low_s[idx], gup_s[...])[:used]
            g_b_down[...] += dot_tn(unfold(c_s[idx], mask_rows), g_in[idx])[:used]

        @pl.when(step >= 3)
        def _():
            unit = at(step - 3)

            @pl.when(is_end)
            def _():
                l_copy(unit).wait_recv()

            _, normed = normed_of(h_in[unit].astype(F32))
            g_a_up[...] += dot_tn(unfold(l_s[unit], mask[unit]), normed)[:used]

        return carry

    lax.fori_loop(0, units + 3, bwd_iter, 0)
    g_b_up[...] = LORA_SCALE * g_b_up[...]
    g_b_down[...] = LORA_SCALE * g_b_down[...]

    @pl.when(is_mid & is_last)
    def _():
        loss_copy_same().start()

    @pl.when(jnp.logical_not(is_mid & is_last))
    def _():
        loss_copy(0).wait_recv()
        loss_out[...] = loss_in[...]

    @pl.when(is_mid & (stage > 0))
    def _():
        loss_copy(0).start()
        loss_copy(1).start()

    @pl.when(is_mid & is_last)
    def _():
        loss_copy_same().wait_send()

    @pl.when(is_mid & (stage > 0))
    def _():
        loss_copy(0).wait_send()
        loss_copy(1).wait_send()

    for unit in (units - 2, units - 1):
        slot = jnp.int32(unit % 2)

        @pl.when(is_end)
        def _():
            part_copy(unit, slot).wait_send()
            part_low_copy(unit, slot).wait_send()
            part_low_copy(unit, slot + 2).wait_send()

            @pl.when(stage > 0)
            def _():
                part_copy(unit, slot + 2).wait_send()

        @pl.when(is_mid)
        def _():
            sum_copy(unit, slot).wait_send()
            sum_low_copy(unit, slot).wait_send()
            sum_low_copy(unit, slot + 2).wait_send()

            @pl.when(stage < last)
            def _():
                hidden_copy(unit, slot, 0).wait_send()
                hidden_copy(unit, slot, 1).wait_send()

            @pl.when(stage > 0)
            def _():
                sum_copy(unit, slot + 2).wait_send()
                grad_copy(unit, slot + 2, 0).wait_send()
                grad_copy(unit, slot + 2, 1).wait_send()

    @pl.when(is_mid)
    def _():
        def drain(idx, carry):
            c_copy(idx).wait_send()
            l_copy(idx).wait_send()

            @pl.when(is_last)
            def _():
                top_copy(idx).wait_send()

            return carry

        lax.fori_loop(0, units, drain, 0)


def sweep(units, stages, weights, rows, mask, weight, collective_id):
    width, d_model = weights[0].shape
    used = weights[4].shape[0]
    msg = d_model + FOLD
    vmem = pl.BlockSpec(memory_space=pltpu.VMEM)
    out_shape = (
        jax.ShapeDtypeStruct((8, LANES), F32),
        jax.ShapeDtypeStruct((used, d_model), F32),
        jax.ShapeDtypeStruct((used, width), F32),
        jax.ShapeDtypeStruct((used, width), F32),
        jax.ShapeDtypeStruct((used, d_model), F32),
    )
    dma = pltpu.SemaphoreType.DMA
    return pl.pallas_call(
        functools.partial(sweep_kernel, units, stages),
        out_shape=out_shape,
        in_specs=[vmem] * 4 + [pl.BlockSpec(memory_space=pltpu.HBM)] * 5 + [vmem] * 2,
        out_specs=(vmem,) * 5,
        scratch_shapes=[
            pltpu.VMEM((units, UNIT, d_model), BF16),
            pltpu.VMEM((units, UNIT, d_model), BF16),
            pltpu.VMEM((units, UNIT, width), F32),
            pltpu.VMEM((units, UNIT, width), F32),
            pltpu.VMEM((units, UNIT, LANES), BF16),
            pltpu.VMEM((units, UNIT, FOLD), BF16),
            pltpu.VMEM((units, UNIT, FOLD), BF16),
            pltpu.VMEM((units, UNIT, d_model), BF16),
            pltpu.VMEM((units, UNIT, FOLD), BF16),
            pltpu.VMEM((2 * units, UNIT, d_model), BF16),
            pltpu.VMEM((2 * units, UNIT, FOLD), BF16),
            pltpu.VMEM((2, UNIT, msg), F32),
            pltpu.VMEM((4, UNIT, d_model), BF16),
            pltpu.VMEM((4, UNIT, FOLD), BF16),
            pltpu.VMEM((4, UNIT, d_model), BF16),
            pltpu.VMEM((4, UNIT, FOLD), BF16),
            pltpu.VMEM((4, UNIT, d_model), BF16),
            pltpu.VMEM((UNIT, width), BF16),
            pltpu.VMEM((UNIT, width), BF16),
            pltpu.VMEM((UNIT, LANES), BF16),
            pltpu.VMEM((8, LANES), F32),
            pltpu.VMEM((LANES, d_model), BF16),
            pltpu.VMEM((LANES, width), BF16),
            pltpu.VMEM((LANES, width), BF16),
            pltpu.VMEM((LANES, d_model), BF16),
            dma,
            dma((4,)),
            dma((units,)),
            dma((units,)),
            dma((2 * units,)),
            dma((2 * units,)),
            dma((units,)),
            dma((units,)),
            dma((units,)),
            dma((units,)),
            dma,
            dma((4,)),
            dma((4,)),
            dma((4,)),
            dma((4,)),
            dma((4, 2)),
            dma((units,)),
            dma((units,)),
            dma((units,)),
            dma((3,)),
        ],
        compiler_params=pltpu.CompilerParams(collective_id=collective_id, has_side_effects=True,
                                             vmem_limit_bytes=66_000_000),
    )(*weights, rows, mask, weight)


def solution(mesh):
    num_stages = mesh.shape["pp"]

    def stage_body(w_gate, w_up, w_down, norm_gain, a_up, b_up, a_down, b_down, inputs, targets, lengths):
        stage_idx = lax.axis_index("pp")
        num_jobs, num_micro, row_count, seq_len, d_model = inputs.shape
        rank = a_up.shape[-1]
        job_rows = num_micro * row_count
        num_rows = num_jobs * job_rows
        num_tokens = num_rows * seq_len
        width = w_gate.shape[-1]
        used = num_jobs * rank

        order = np.arange(num_rows).reshape(lengths.shape)
        row_lens = jnp.sum(jnp.where(np.arange(num_rows)[:, None, None, None] == order[None], lengths[None], 0), axis=(1, 2, 3))
        row_ends = jnp.cumsum(row_lens)
        row_starts = row_ends - row_lens
        job_norms = jnp.sum(lengths, axis=(1, 2)).astype(F32) * d_model
        row_jobs = jnp.arange(num_rows) // job_rows
        row_shift = jnp.arange(num_rows) * seq_len - row_starts
        row_weight = jnp.repeat(1.0 / job_norms, job_rows)

        a_up_all = jnp.swapaxes(a_up[0], 1, 2).reshape(used, d_model)
        b_up_all = b_up[0].reshape(used, width)
        a_down_all = jnp.swapaxes(a_down[0], 1, 2).reshape(used, width)
        b_down_all = b_down[0].reshape(used, d_model)
        gain = jnp.broadcast_to(norm_gain.astype(F32), (UNIT, d_model))
        weights = (jnp.swapaxes(w_gate[0], 0, 1), jnp.swapaxes(w_up[0], 0, 1), w_down[0], gain, a_up_all, b_up_all, a_down_all, b_down_all)
        rows_all = jnp.where(stage_idx == num_stages - 1, targets, inputs).reshape(num_tokens, d_model)

        def run(plan):
            def one_pass(units, first):
                slots = first + jnp.arange(units * UNIT)
                in_row = (slots[:, None] >= row_starts[None, :]) & (slots[:, None] < row_ends[None, :])
                valid = slots < row_ends[-1]
                source = slots + jnp.sum(jnp.where(in_row, row_shift[None, :], 0), axis=1)
                job = jnp.sum(jnp.where(in_row, row_jobs[None, :], 0), axis=1)
                weight = jnp.sum(jnp.where(in_row, row_weight[None, :], 0.0), axis=1)
                pick = ((source[:, None] == jnp.arange(num_tokens)[None, :]) & valid[:, None]).astype(BF16)
                rows = jnp.dot(pick, rows_all, preferred_element_type=F32).astype(BF16)
                mask = ((jnp.arange(LANES)[None, :] // rank == job[:, None]) & valid[:, None]).astype(BF16)
                return sweep(units, num_stages, weights,
                             rows.reshape(units, UNIT, d_model), mask.reshape(units, UNIT, LANES),
                             jnp.broadcast_to(weight[:, None], (units * UNIT, FOLD)).reshape(units, UNIT, FOLD), 0)

            if len(plan) == 1:
                return tuple(one_pass(plan[0], 0))
            zeros = tuple(jnp.zeros(shape, F32) for shape in ((8, LANES), (used, d_model), (used, width), (used, width), (used, d_model)))
            return lax.fori_loop(0, len(plan), lambda turn, outs: tuple(
                old + add for old, add in zip(outs, one_pass(plan[0], turn * plan[0] * UNIT))), zeros)

        caps = [sum(plan) * UNIT for plan in PLANS]
        choice = sum((row_ends[-1] > cap).astype(jnp.int32) for cap in caps[:-1])
        loss, g_a_up, g_b_up, g_a_down, g_b_down = lax.switch(choice, [functools.partial(run, plan) for plan in PLANS])
        losses = 0.5 * loss[0, :used:rank]
        g_a_up = jnp.swapaxes(g_a_up.reshape(1, num_jobs, rank, d_model), 2, 3)
        g_b_up = g_b_up.reshape(1, num_jobs, rank, width)
        g_a_down = jnp.swapaxes(g_a_down.reshape(1, num_jobs, rank, width), 2, 3)
        g_b_down = g_b_down.reshape(1, num_jobs, rank, d_model)
        return losses, g_a_up, g_b_up, g_a_down, g_b_down

    weight_specs = (P("pp", None, "tp"), P("pp", None, "tp"), P("pp", "tp", None), P("pp", None))
    adapter_specs = (P("pp", "rep", None, None), P("pp", "rep", None, "tp"), P("pp", "rep", "tp", None), P("pp", "rep", None, None))
    data_specs = (P("rep"), P("rep"), P("rep"))
    return jax.shard_map(stage_body, mesh=mesh, in_specs=weight_specs + adapter_specs + data_specs,
                         out_specs=(P("rep"),) + adapter_specs, check_vma=False)
```
